768 devices in a mesh: grp: 48 (over y_lo, z), blk: 16 (over y_hi, x, core).
Axes of the slice: x: 4, y: 8 (y_hi: 2, y_lo: 4; y = y_hi * 4 + y_lo), z: 12, core: 2. Of those that a mesh axis runs over, the one named last changes fastest.
Arguments:
- query: bfloat16 [98304, 512], P(('grp', 'blk')), may hold values from -6 to 6
- key: bfloat16 [98304, 512], P(('grp', 'blk')), may hold values from -6 to 6
- value: bfloat16 [98304, 512], P(('grp', 'blk')), may hold values from -6 to 6
- gate_u: bfloat16 [98304, 512], P(('grp', 'blk')), may hold values from -6 to 6
- out_grad: bfloat16 [98304, 1024], P(('grp', 'blk')), may hold values from -6 to 6
- lengths: int32 [48], P('grp'), may hold values from 32 to 2048
- norm_gain: float32 [512], replicated, may hold values from 0.1 to 1.9
- out_weight: bfloat16 [512, 1024], replicated, may hold values from -0.25 to 0.25
Outputs:
- layer_out: bfloat16 [98304, 1024], P(('grp', 'blk'))
- grad_query: bfloat16 [98304, 512], P(('grp', 'blk'))
- grad_key: bfloat16 [98304, 512], P(('grp', 'blk'))
- grad_value: bfloat16 [98304, 512], P(('grp', 'blk'))
- grad_gate: bfloat16 [98304, 512], P(('grp', 'blk'))
- grad_weight: float32 [512, 1024], P(None, 'blk')
The draws below stay inside these ranges and needn't reach their ends.
Inputs may be any that keep to these rules, and one draw needn't show every extreme that they name: `lengths`: events of a user at or past its length are padding.
All inputs are finite; a program needn't handle non-finite values.
Results may differ from the reference program's by a relative error of at most 0.009.
Values may be sent and summed in bfloat16 or wider, within the bound.
A program may use at most 64 MiB of HBM per device.

```python
from functools import partial
import jax
import jax.numpy as jnp
from jax import lax

D = 1024
HEADS = 8
HEAD = 64
HD = 512
NSEQ = 2048
USERS = 48
TOKENS = 98304


def plant(entries, rng, smallest, top_value):
    longest = entries.shape.index(max(entries.shape))
    spots = []
    for shift in (0, 1):
        where = [jax.random.randint(jax.random.fold_in(rng, axis), (), 0, length) for axis, length in enumerate(entries.shape)]
        where[longest] = (where[longest] + shift) % entries.shape[longest]
        spots.append(tuple(where))
    return entries.at[spots[0]].set(smallest).at[spots[1]].set(top_value)


def block_levels(rng, dims, cuts, low, largest):
    level, own = 1.0, jax.random.fold_in(rng, 6)
    for dim, shards_of in cuts:
        draws = jnp.exp(jax.random.uniform(jax.random.fold_in(own, dim), (shards_of,), jnp.float32, low / len(cuts), largest / len(cuts)))
        level = level * jnp.repeat(draws, dims[dim] // shards_of).reshape([-1 if axis == dim else 1 for axis in range(len(dims))])
    return level


def noise(key, shape, scale, bound, cuts=(), kind=jnp.bfloat16):
    result = scale * jax.random.normal(key, shape, jnp.float32)
    if cuts:
        result = result * block_levels(key, shape, cuts, -0.22, 0.18)
    return jnp.clip(result, -bound, bound).astype(kind)


def setup_inputs(seed: int = 0) -> dict:
    key_of = jax.random.split(jax.random.key(seed), 9)
    return {
        "query": noise(key_of[0], (TOKENS, HD), 1.0, 6.0, ((0, 768),)),
        "key": noise(key_of[1], (TOKENS, HD), 1.0, 6.0, ((0, 768),)),
        "value": noise(key_of[2], (TOKENS, HD), 1.0, 6.0, ((0, 768),)),
        "gate_u": noise(key_of[3], (TOKENS, HD), 1.0, 6.0, ((0, 768),)),
        "out_grad": noise(key_of[4], (TOKENS, D), 1.0, 6.0, ((0, 768),)),
        "lengths": plant(jax.random.randint(key_of[5], (USERS,), min(32, NSEQ // 2), NSEQ + 1), jax.random.fold_in(key_of[5], 1), min(32, NSEQ // 2), NSEQ).astype(jnp.int32),
        "norm_gain": jnp.clip(1.0 + 0.18 * jax.random.normal(key_of[6], (HD,), jnp.float32), 0.1, 1.9),
        "out_weight": noise(key_of[7], (HD, D), HD ** -0.5, 0.25),
    }


EPS = 1e-05

def user_pass(norm_gain, weight_mat, total, items):
    queries, keys_in, values_in, gates, cotangent, length = items
    count = queries.shape[0]
    scale = HEAD ** (-0.5)
    places = jnp.arange(count, dtype=jnp.int32)
    alive = places < length
    mask = (places[None, :] <= places[:, None]) & alive[:, None] & alive[None, :]
    query_heads = queries.astype(jnp.float32).reshape(count, HEADS, HEAD)
    key_heads = keys_in.astype(jnp.float32).reshape(count, HEADS, HEAD)
    value_heads = values_in.astype(jnp.float32).reshape(count, HEADS, HEAD)
    scores = jnp.einsum('ihd,jhd->hij', query_heads, key_heads) * scale
    weights = (jax.nn.silu(scores) * mask[None]).astype(jnp.bfloat16)
    attended = jnp.einsum('hij,jhd->ihd', weights.astype(jnp.float32), value_heads).reshape(count, HEADS * HEAD)
    centre = attended - lax.optimization_barrier(jnp.mean(attended, axis=1, keepdims=True))
    inv_std = lax.rsqrt(lax.optimization_barrier(jnp.mean(centre * centre, axis=1, keepdims=True)) + EPS)
    normed = centre * inv_std
    scaled = normed * norm_gain
    mixed = (scaled * gates.astype(jnp.float32)).astype(jnp.bfloat16)
    layer_out = jnp.dot(mixed, weight_mat, preferred_element_type=jnp.float32).astype(jnp.bfloat16)
    mixed_grad = jnp.dot(cotangent, weight_mat.T, preferred_element_type=jnp.float32)
    grad_gate = (mixed_grad * scaled).astype(jnp.bfloat16)
    normed_grad = mixed_grad * gates.astype(jnp.float32) * norm_gain
    attended_grad = inv_std * (normed_grad - lax.optimization_barrier(jnp.mean(normed_grad, axis=1, keepdims=True)) - normed * lax.optimization_barrier(jnp.mean(normed_grad * normed, axis=1, keepdims=True)))
    attended_grad = attended_grad.astype(jnp.bfloat16)
    grad_heads = attended_grad.astype(jnp.float32).reshape(count, HEADS, HEAD)
    prob_grad = jnp.einsum('ihd,jhd->hij', grad_heads, value_heads)
    sigma = jax.nn.sigmoid(scores)
    score_grad = (prob_grad * sigma * (1.0 + scores * (1.0 - sigma)) * mask[None]).astype(jnp.bfloat16).astype(jnp.float32)
    grad_query = (jnp.einsum('hij,jhd->ihd', score_grad, key_heads) * scale).reshape(count, HEADS * HEAD).astype(jnp.bfloat16)
    grad_key = (jnp.einsum('hij,ihd->jhd', score_grad, query_heads) * scale).reshape(count, HEADS * HEAD).astype(jnp.bfloat16)
    grad_value = jnp.einsum('hij,ihd->jhd', weights.astype(jnp.float32), grad_heads).reshape(count, HEADS * HEAD).astype(jnp.bfloat16)
    weight_term = jnp.dot(mixed.T, cotangent, preferred_element_type=jnp.float32)
    return (total + weight_term, (layer_out, grad_query, grad_key, grad_value, grad_gate))

def reference(query, key, value, gate_u, out_grad, lengths, norm_gain, out_weight):

    def shaped(array):
        return array.reshape(USERS, NSEQ, array.shape[-1])

    def flatten(array):
        return array.reshape(TOKENS, array.shape[-1])
    start_total = jnp.zeros((HEADS * HEAD, D), jnp.float32)
    stepper = partial(user_pass, norm_gain, out_weight)
    total, results = lax.scan(stepper, start_total, (shaped(query), shaped(key), shaped(value), shaped(gate_u), shaped(out_grad), lengths))
    layer_out, grad_query, grad_key, grad_value, grad_gate = results
    return (flatten(layer_out), flatten(grad_query), flatten(grad_key), flatten(grad_value), flatten(grad_gate), total)
```

```python
import math

import jax
import jax.numpy as jnp
from jax import lax
from jax.experimental import pallas as pl
from jax.experimental.pallas import tpu as pltpu
from jax.sharding import PartitionSpec as P

HEADS = 8
HEAD = 64


EPS = 1e-05


MESH = pl.DeviceIdType.MESH
NZ = 12
NYL = 4
NX = 4


def where_am_i():
    g, b = (lax.axis_index("grp"), lax.axis_index("blk"))
    return (g // NZ, g % NZ, b // 8, (b // 2) % NX, b % 2)


def device(y_lo, z, y_hi, x, core):
    return (y_lo * NZ + z, (y_hi * NX + x) * 2 + core)


def remote(src, dst, send_sem, recv_sem, target):
    return pltpu.make_async_remote_copy(
        src_ref=src, dst_ref=dst, send_sem=send_sem, recv_sem=recv_sem,
        device_id=target, device_id_type=MESH,
    )


def weight_partners(me):
    y_lo, z, y_hi, x, core = me
    y = y_hi * NYL + y_lo
    found = [device(y_lo, z, y_hi, x, 1 - core)]
    for d in range(1, NX):
        found.append(device(y_lo, z, y_hi, (x + d) % NX, core))
    for d in range(1, 8):
        to = (y + d) % 8
        found.append(device(to % NYL, z, to // NYL, x, core))
    for d in range(1, NZ):
        found.append(device(y_lo, (z + d) % NZ, y_hi, x, core))
    return found


def weight_kernel(
    mixed_ref, cot_ref, out_ref,
    term, term_send, core_got, x_own, x_send, x_got, y_own, y_send, y_got, z_all, gathered,
    core_sem, x_ssem, x_rsem, y_ssem, y_rsem, z_ssem, z_rsem, g_ssem, g_rsem,
):
    me = where_am_i()
    y_lo, z, y_hi, x, core = me
    y = y_hi * NYL + y_lo
    barrier = pltpu.get_barrier_semaphore()
    partners = weight_partners(me)
    for target in partners:
        pl.semaphore_signal(barrier, inc=1, device_id=target, device_id_type=MESH)

    mixed = mixed_ref[...]
    for hi in range(2):
        for xx in range(NX):
            block = hi * NX + xx
            part = lax.dot_general(
                cot_ref[:, block * 128:(block + 1) * 128], mixed,
                (((0,), (0,)), ((), ())), preferred_element_type=jnp.float32,
            )
            for cc in range(2):
                piece = part[cc * 64:(cc + 1) * 64]
                term[cc, xx, hi] = piece
                term_send[cc, xx, hi] = piece.astype(jnp.bfloat16)
    pl.semaphore_wait(barrier, len(partners))

    to_core = remote(
        term_send.at[1 - core], core_got, core_sem.at[0], core_sem.at[1],
        device(y_lo, z, y_hi, x, 1 - core),
    )
    to_core.start()
    to_core.wait_recv()
    sends = [to_core]
    for d in range(1, NX):
        xx = (x + d) % NX
        x_send[d] = (term[core, xx] + core_got[xx].astype(jnp.float32)).astype(jnp.bfloat16)
        copy = remote(
            x_send.at[d], x_got.at[d], x_ssem.at[d], x_rsem.at[d],
            device(y_lo, z, y_hi, xx, core),
        )
        copy.start()
        sends.append(copy)
    x_own[...] = term[core, x] + core_got[x].astype(jnp.float32)
    for d in range(1, NX):
        sends[d].wait_recv()
        x_own[...] += x_got[d].astype(jnp.float32)
    for hi in range(2):
        for lo in range(NYL):
            piece = x_own[hi, lo * 16:(lo + 1) * 16]
            y_own[hi * NYL + lo] = piece
            y_send[hi * NYL + lo] = piece.astype(jnp.bfloat16)
    to_y = []
    for d in range(1, 8):
        to = (y + d) % 8
        copy = remote(
            y_send.at[to], y_got.at[d], y_ssem.at[d], y_rsem.at[d],
            device(to % NYL, z, to // NYL, x, core),
        )
        copy.start()
        to_y.append(copy)
    total = y_own[y]
    for d in range(1, 8):
        to_y[d - 1].wait_recv()
        total = total + y_got[d].astype(jnp.float32)
    z_all[z] = total.astype(jnp.bfloat16)
    to_z = []
    for d in range(1, NZ):
        copy = remote(
            z_all.at[z], z_all.at[z], z_ssem.at[d], z_rsem.at[d],
            device(y_lo, (z + d) % NZ, y_hi, x, core),
        )
        copy.start()
        to_z.append(copy)
    for d in range(1, NZ):
        remote(
            z_all.at[z], z_all.at[(z + NZ - d) % NZ], z_ssem.at[d], z_rsem.at[d],
            device(y_lo, (z + d) % NZ, y_hi, x, core),
        ).wait_recv()
    total = z_all[0].astype(jnp.float32)
    for zz in range(1, NZ):
        total = total + z_all[zz].astype(jnp.float32)
    gathered[y_lo] = total
    to_g = []
    for d in range(1, NYL):
        copy = remote(
            gathered.at[y_lo], gathered.at[y_lo], g_ssem.at[d], g_rsem.at[d],
            device((y_lo + d) % NYL, z, y_hi, x, core),
        )
        copy.start()
        to_g.append(copy)
    for d in range(1, NYL):
        remote(
            gathered.at[y_lo], gathered.at[(y_lo + NYL - d) % NYL], g_ssem.at[d], g_rsem.at[d],
            device((y_lo + d) % NYL, z, y_hi, x, core),
        ).wait_recv()
    out_ref[...] = gathered[...].reshape(64, 512).T
    for copy in sends + to_y + to_z + to_g:
        copy.wait_send()


def weight_reduce(mixed, cotangent):
    f32, bf16, dma = (jnp.float32, jnp.bfloat16, pltpu.SemaphoreType.DMA)
    vmem = pltpu.VMEM
    return pl.pallas_call(
        weight_kernel,
        out_shape=jax.ShapeDtypeStruct((512, 64), f32),
        in_specs=[pl.BlockSpec(memory_space=vmem)] * 2,
        out_specs=pl.BlockSpec(memory_space=vmem),
        scratch_shapes=[
            vmem((2, NX, 2, 64, 512), f32),
            vmem((2, NX, 2, 64, 512), bf16),
            vmem((NX, 2, 64, 512), bf16),
            vmem((2, 64, 512), f32),
            vmem((NX, 2, 64, 512), bf16),
            vmem((NX, 2, 64, 512), bf16),
            vmem((8, 16, 512), f32),
            vmem((8, 16, 512), bf16),
            vmem((8, 16, 512), bf16),
            vmem((NZ, 16, 512), bf16),
            vmem((NYL, 16, 512), f32),
            dma((2,)), dma((NX,)), dma((NX,)), dma((8,)), dma((8,)),
            dma((NZ,)), dma((NZ,)), dma((NYL,)), dma((NYL,)),
        ],
        compiler_params=pltpu.CompilerParams(collective_id=0, has_side_effects=True),
    )(mixed, cotangent)


def in_one_piece(arrays, axis, split_dim, concat_dim, along):
    ends, at = ([], 0)
    for a in arrays[:-1]:
        at += a.shape[along]
        ends.append(at)
    both = jnp.concatenate(arrays, axis=along)
    return tuple(
        jnp.split(
            lax.all_to_all(both, axis, split_axis=split_dim, concat_axis=concat_dim, tiled=True),
            ends,
            axis=along,
        )
    )


def causal_mask(query_pos, key_pos, length):
    return (
        (key_pos[None, :] <= query_pos[:, None])
        & (query_pos[:, None] < length)
        & (key_pos[None, :] < length)
    )


def over_blocks(total_rows, step_fn, initial):
    size = math.gcd(total_rows, 512)

    def advance(index, carry):
        return step_fn(carry, index * size, size)

    return lax.fori_loop(0, total_rows // size, advance, initial)


def guarded(is_live, work, carry):
    return lax.cond(is_live, work, lambda held: held, carry)


def shards(query, key, value, gate_u, out_grad, lengths, norm_gain, out_weight):
    rows = query.shape[0]
    scale = HEAD ** (-0.5)
    length = lengths[0]
    lanes = lax.axis_size("blk")
    position = lax.axis_index("blk")
    per_head = max(1, lanes // HEADS)
    heads_dev = max(1, HEADS // lanes)
    head_groups = HEADS // heads_dev
    feats = heads_dev * HEAD
    stripe = rows // per_head
    member = position % per_head
    total_len = rows * lanes

    def rows_to_heads(array):
        parts = array.reshape(per_head, stripe, head_groups, feats).transpose(1, 2, 0, 3)
        return parts.reshape(stripe, lanes, feats)

    def heads_to_rows(array):
        parts = array.reshape(stripe, head_groups, per_head, feats).transpose(2, 0, 1, 3)
        return parts.reshape(rows, HEADS * HEAD)

    key_send = jnp.repeat(key.reshape(rows, head_groups, feats), per_head, axis=1)
    value_send = jnp.repeat(value.reshape(rows, head_groups, feats), per_head, axis=1)
    keys_mine, values_mine = in_one_piece((key_send, value_send), "blk", 1, 0, 2)
    query_mine = lax.all_to_all(
        rows_to_heads(query), "blk", split_axis=1, concat_axis=0, tiled=True
    )
    mine_pos = (
        jnp.arange(lanes, dtype=jnp.int32)[:, None] * rows
        + member * stripe
        + jnp.arange(stripe, dtype=jnp.int32)[None, :]
    ).reshape(lanes * stripe)
    mine_low = member * stripe
    mine_high = (lanes - 1) * rows + (member + 1) * stripe - 1
    mine_zero = jnp.zeros((lanes * stripe, heads_dev, HEAD), jnp.float32)

    def heads_live(begin):
        return (begin <= mine_high) & (begin < length) & (mine_low < length)

    def head_forward(carry, begin, size):

        def work(held):
            key_block = lax.dynamic_slice_in_dim(keys_mine, begin, size, 0)
            value_block = lax.dynamic_slice_in_dim(values_mine, begin, size, 0)
            scores = (
                jnp.einsum(
                    "rhd,nhd->hrn", query_mine, key_block, preferred_element_type=jnp.float32
                )
                * scale
            )
            mask = causal_mask(mine_pos, begin + jnp.arange(size, dtype=jnp.int32), length)
            weights = (jax.nn.silu(scores) * mask[None]).astype(jnp.bfloat16)
            return held + jnp.einsum(
                "hrn,nhd->rhd", weights, value_block, preferred_element_type=jnp.float32
            )

        return guarded(heads_live(begin), work, carry)

    attended_mine = over_blocks(total_len, head_forward, mine_zero)
    attended_back = lax.all_to_all(attended_mine, "blk", split_axis=0, concat_axis=1, tiled=True)
    attended = heads_to_rows(attended_back)
    centre = attended - jnp.mean(attended, axis=1, keepdims=True)
    inv_std = lax.rsqrt(jnp.mean(centre * centre, axis=1, keepdims=True) + EPS)
    normed = centre * inv_std
    scaled = normed * norm_gain
    gates = gate_u.astype(jnp.float32)
    mixed = (scaled * gates).astype(jnp.bfloat16)
    layer_out = jnp.dot(mixed, out_weight, preferred_element_type=jnp.float32).astype(jnp.bfloat16)
    mixed_grad = lax.dot_general(
        out_grad, out_weight, (((1,), (1,)), ((), ())), preferred_element_type=jnp.float32
    )
    grad_gate = (mixed_grad * scaled).astype(jnp.bfloat16)
    normed_grad = mixed_grad * gates * norm_gain
    attended_grad = inv_std * (
        normed_grad
        - jnp.mean(normed_grad, axis=1, keepdims=True)
        - normed * jnp.mean(normed_grad * normed, axis=1, keepdims=True)
    )
    attended_grad = attended_grad.astype(jnp.bfloat16)
    grad_mine = lax.all_to_all(
        rows_to_heads(attended_grad), "blk", split_axis=1, concat_axis=0, tiled=True
    )
    full_zero = jnp.zeros((total_len, heads_dev, HEAD), jnp.float32)

    def head_backward(carry, begin, size):

        def work(held):
            query_acc, key_full, value_full = held
            key_block = lax.dynamic_slice_in_dim(keys_mine, begin, size, 0)
            value_block = lax.dynamic_slice_in_dim(values_mine, begin, size, 0)
            scores = (
                jnp.einsum(
                    "rhd,nhd->hrn", query_mine, key_block, preferred_element_type=jnp.float32
                )
                * scale
            )
            mask = causal_mask(mine_pos, begin + jnp.arange(size, dtype=jnp.int32), length)
            weights = (jax.nn.silu(scores) * mask[None]).astype(jnp.bfloat16)
            sigma = jax.nn.sigmoid(scores)
            prob_grad = jnp.einsum(
                "rhd,nhd->hrn", grad_mine, value_block, preferred_element_type=jnp.float32
            )
            score_grad = (prob_grad * sigma * (1.0 + scores * (1.0 - sigma)) * mask[None]).astype(
                jnp.bfloat16
            )
            query_acc = query_acc + jnp.einsum(
                "hrn,nhd->rhd", score_grad, key_block, preferred_element_type=jnp.float32
            )
            key_part = jnp.einsum(
                "hrn,rhd->nhd", score_grad, query_mine, preferred_element_type=jnp.float32
            )
            value_part = jnp.einsum(
                "hrn,rhd->nhd", weights, grad_mine, preferred_element_type=jnp.float32
            )
            key_full = lax.dynamic_update_slice_in_dim(key_full, key_part, begin, 0)
            value_full = lax.dynamic_update_slice_in_dim(value_full, value_part, begin, 0)
            return (query_acc, key_full, value_full)

        return guarded(heads_live(begin), work, carry)

    query_acc, key_full, value_full = over_blocks(
        total_len, head_backward, (mine_zero, full_zero, full_zero)
    )
    query_send = (query_acc * scale).astype(jnp.bfloat16)
    grad_query = heads_to_rows(
        lax.all_to_all(query_send, "blk", split_axis=0, concat_axis=1, tiled=True)
    )
    key_back, value_back = tuple(
        (
            part.astype(jnp.float32)
            for part in in_one_piece(
                (key_full.astype(jnp.bfloat16), value_full.astype(jnp.bfloat16)), "blk", 0, 1, 2
            )
        )
    )
    key_sum = (
        key_back.reshape(rows, head_groups, per_head, feats).sum(axis=2).reshape(rows, HEADS * HEAD)
    )
    value_sum = (
        value_back.reshape(rows, head_groups, per_head, feats)
        .sum(axis=2)
        .reshape(rows, HEADS * HEAD)
    )
    grad_key = (key_sum * scale).astype(jnp.bfloat16)
    grad_value = value_sum.astype(jnp.bfloat16)
    grad_weight = weight_reduce(mixed, out_grad)
    return (layer_out, grad_query, grad_key, grad_value, grad_gate, grad_weight)


def solution(mesh):
    return jax.shard_map(
        shards,
        mesh=mesh,
        in_specs=(
            P(("grp", "blk"), None),
            P(("grp", "blk"), None),
            P(("grp", "blk"), None),
            P(("grp", "blk"), None),
            P(("grp", "blk"), None),
            P("grp"),
            P(),
            P(),
        ),
        out_specs=(
            P(("grp", "blk"), None),
            P(("grp", "blk"), None),
            P(("grp", "blk"), None),
            P(("grp", "blk"), None),
            P(("grp", "blk"), None),
            P(None, "blk"),
        ),
        check_vma=False,
    )
```

```python
import jax
import jax.numpy as jnp
from jax import lax
from jax.experimental import pallas as pl
from jax.experimental.pallas import tpu as pltpu
from jax.sharding import PartitionSpec as P

MESH = pl.DeviceIdType.MESH
EPS = 1e-05
NZ = 12
NYL = 4
NX = 4
HALF = 8
ROWS = 128
TILE = 512
PIECE = 64 // NYL
F32 = jnp.float32
BF16 = jnp.bfloat16


def where_am_i():
    g, b = (lax.axis_index("grp"), lax.axis_index("blk"))
    return (g // NZ, g % NZ, b // 8, (b // 2) % NX, b % 2)


def device(y_lo, z, y_hi, x, core):
    return (y_lo * NZ + z, (y_hi * NX + x) * 2 + core)


def remote(src, dst, send_sem, recv_sem, target):
    return pltpu.make_async_remote_copy(
        src_ref=src, dst_ref=dst, send_sem=send_sem, recv_sem=recv_sem,
        device_id=target, device_id_type=MESH,
    )


def all_partners(me):
    y_lo, z, y_hi, x, core = me
    g = y_lo * NZ + z
    mine = (y_hi * NX + x) * 2 + core
    y = y_hi * NYL + y_lo
    found = [(g, (mine + d) % 16) for d in range(1, 16)]
    for d in range(1, 2 * NYL):
        if d != NYL:
            to = (y + d) % (2 * NYL)
            found.append(device(to % NYL, z, to // NYL, x, core))
    for d in range(1, NZ):
        found.append(device(y_lo, (z + d) % NZ, y_hi, x, core))
    return found


def swap(part):
    return pltpu.roll(part.astype(F32), 64, 1)


def low_lanes(rows):
    return lax.broadcasted_iota(jnp.int32, (rows, 128), 1) < 64


def fold_rows(block, odd):
    low = low_lanes(64)
    top, bottom = (block[:64], block[64:])
    if odd:
        return jnp.where(low, swap(top), bottom.astype(F32))
    return jnp.where(low, top.astype(F32), swap(bottom))


def join_heads(even, odd):
    low = low_lanes(even.shape[0])
    return (jnp.where(low, even, swap(odd)), jnp.where(low, swap(even), odd))


def nt(left, right):
    return lax.dot_general(left, right, (((1,), (1,)), ((), ())), preferred_element_type=F32)


def tn(left, right):
    return lax.dot_general(left, right, (((0,), (0,)), ((), ())), preferred_element_type=F32)


def nn(left, right):
    return jnp.dot(left, right, preferred_element_type=F32)


def layer_kernel(
    q_ref, k_ref, v_ref, gate_ref, cot_ref, length_ref, gain_ref, weight_ref,
    out_ref, gq_ref, gk_ref, gv_ref, gg_ref, gw_ref,
    in_send, in_got, up_got, qf, dof, att_acc, att_send, att_got, do_send, do_got,
    dkv_acc, dqt_acc, up_acc, back_send, back_got, down_send, down_got, mixed_grad, scaled_buf,
    mixed_buf,
    term, term_send, core_got, x_own, x_send, x_got, y_own, y_send, y_got, z_all, gathered,
    in_ss, in_rs, up_ss, up_rs, att_ss, att_rs, do_ss, do_rs, back_ss, back_rs, down_ss, down_rs,
    core_sem, x_ssem, x_rsem, y_ssem, y_rsem, z_ssem, z_rsem, g_ssem, g_rsem,
):
    me = where_am_i()
    y_lo, z, y_hi, x, core = me
    g = y_lo * NZ + z
    y = y_hi * NYL + y_lo
    h = x * 2 + core
    base = y_hi * HALF
    upper = y_hi == 1
    lower = y_hi == 0

    barrier = pltpu.get_barrier_semaphore()
    partners = all_partners(me)
    for target in partners:
        pl.semaphore_signal(barrier, inc=1, device_id=target, device_id_type=MESH)

    low128 = low_lanes(128)
    for t in range(HALF):
        cols = slice((t // 2) * 128, (t // 2 + 1) * 128)
        kk, vv = (k_ref[:, cols], v_ref[:, cols])
        if t % 2:
            pair = jnp.where(low128, swap(kk), vv.astype(F32))
        else:
            pair = jnp.where(low128, kk.astype(F32), swap(vv))
        in_send[t, 64:192] = pair.astype(BF16)
        in_send[t, 0:64] = (fold_rows(q_ref[:, cols], t % 2) * 0.0625).astype(BF16)
    in_got[h] = in_send[h]
    pl.semaphore_wait(barrier, len(partners))

    def up_copy(t):
        return remote(
            in_send.at[t, pl.ds(64, 128)], up_got.at[h], up_ss.at[t], up_rs.at[h], (g, HALF + t)
        )

    def up_arrival(s):
        return remote(
            in_send.at[s, pl.ds(64, 128)], up_got.at[s], up_ss.at[s], up_rs.at[s], (g, s)
        )

    @pl.when(lower)
    def _():
        for t in range(HALF):
            up_copy(t).start()

    def to_half(send, got, ssem, rsem):
        copies = []
        for d in range(1, HALF):
            t = (h + d) % HALF
            copies.append(remote(send.at[t], got.at[h], ssem.at[d], rsem.at[d], (g, base + t)))
        return copies

    def from_half(send, got, ssem, rsem):
        for d in range(1, HALF):
            t = (h + d) % HALF
            s = (h + HALF - d) % HALF
            remote(send.at[t], got.at[s], ssem.at[d], rsem.at[d], (g, base + t)).wait_recv()

    to_in = to_half(in_send, in_got, in_ss, in_rs)
    for copy in to_in:
        copy.start()
    mixed_grad[...] = nt(cot_ref[...], weight_ref[...])
    from_half(in_send, in_got, in_ss, in_rs)

    low64 = low_lanes(64)
    for s in range(HALF):
        folded = in_got[s, 0:64].astype(F32)
        qf[s * 128:s * 128 + 64] = jnp.where(low64, folded, 0.0).astype(BF16)
        qf[s * 128 + 64:s * 128 + 128] = jnp.where(low64, swap(folded), 0.0).astype(BF16)
    att_acc[...] = jnp.zeros_like(att_acc)

    def local_kv(j):
        return in_got[pl.ds(j * 4, 4), 64:192].reshape(TILE, 128)

    def upper_kv(j):
        return up_got[pl.ds(j * 4, 4)].reshape(TILE, 128)

    def rows_of(i):
        return pl.ds(pl.multiple_of(i * TILE, TILE), TILE)

    tile_row = lax.broadcasted_iota(jnp.int32, (TILE, TILE), 0)
    tile_col = lax.broadcasted_iota(jnp.int32, (TILE, TILE), 1)

    def forward_tile(i, kv, diagonal):
        half_score = nt(qf[rows_of(i)], kv)
        weight = half_score + half_score * jnp.tanh(half_score)
        if diagonal:
            weight = jnp.where(tile_col <= tile_row, weight, 0.0)
        att_acc[rows_of(i)] += nn(weight.astype(BF16), kv)

    @pl.loop(0, 2)
    def _(i):
        forward_tile(i, local_kv(i), True)

    forward_tile(1, local_kv(0), False)

    @pl.when(upper)
    def _():
        for s in range(HALF):
            up_arrival(s).wait_recv()

        @pl.loop(0, 4)
        def _(n):
            forward_tile(n % 2, upper_kv(n // 2), False)

    for s in range(HALF):
        top = att_acc[s * 128:s * 128 + 64]
        bottom = att_acc[s * 128 + 64:s * 128 + 128]
        att_send[s] = jnp.where(low64, swap(top), bottom).astype(BF16)
    att_got[h] = att_send[h]
    to_att = to_half(att_send, att_got, att_ss, att_rs)
    for copy in to_att:
        copy.start()
    from_half(att_send, att_got, att_ss, att_rs)

    blocks = []
    for p in range(HALF // 2):
        even, odd = (att_got[2 * p].astype(F32), att_got[2 * p + 1].astype(F32))
        top, bottom = join_heads(even, odd)
        blocks.append(jnp.concatenate([top, bottom], axis=0))
    attended = jnp.concatenate(blocks, axis=1)
    row = (base + h) * ROWS + lax.broadcasted_iota(jnp.int32, (ROWS, 512), 0)
    alive = row < length_ref[0]
    attended = jnp.where(alive, attended, 0.0)
    centre = attended - jnp.mean(attended, axis=1, keepdims=True)
    inv_std = lax.rsqrt(jnp.mean(centre * centre, axis=1, keepdims=True) + EPS)
    normed = centre * inv_std
    gain = gain_ref[...]
    scaled = normed * gain
    gates = gate_ref[...].astype(F32)
    scaled_buf[...] = scaled
    mixed_buf[...] = (scaled * gates).astype(BF16)
    normed_grad = mixed_grad[...] * gates * gain
    attended_grad = inv_std * (
        normed_grad
        - jnp.mean(normed_grad, axis=1, keepdims=True)
        - normed * jnp.mean(normed_grad * normed, axis=1, keepdims=True)
    )
    attended_grad = jnp.where(alive, attended_grad, 0.0).astype(BF16).astype(F32)
    for t in range(HALF):
        cols = slice((t // 2) * 128, (t // 2 + 1) * 128)
        do_send[t] = fold_rows(attended_grad[:, cols], t % 2).astype(BF16)
    do_got[h] = do_send[h]
    to_do = to_half(do_send, do_got, do_ss, do_rs)
    for copy in to_do:
        copy.start()

    mixed = mixed_buf[...]
    for hi in range(2):
        for xx in range(NX):
            block = hi * NX + xx
            part = tn(cot_ref[:, block * 128:(block + 1) * 128], mixed)
            for cc in range(2):
                piece = part[cc * 64:(cc + 1) * 64]
                term[cc, xx, hi] = piece
                term_send[cc, xx, hi] = piece.astype(BF16)
    to_core = remote(
        term_send.at[1 - core], core_got, core_sem.at[0], core_sem.at[1],
        device(y_lo, z, y_hi, x, 1 - core),
    )
    to_core.start()
    out_ref[...] = nn(mixed, weight_ref[...]).astype(BF16)
    gg_ref[...] = (mixed_grad[...] * scaled_buf[...]).astype(BF16)

    from_half(do_send, do_got, do_ss, do_rs)
    for s in range(HALF):
        folded = do_got[s].astype(F32)
        dof[s * 128:s * 128 + 64] = jnp.where(low64, 0.0, swap(folded)).astype(BF16)
        dof[s * 128 + 64:s * 128 + 128] = jnp.where(low64, 0.0, folded).astype(BF16)
    dkv_acc[...] = jnp.zeros_like(dkv_acc)
    dqt_acc[...] = jnp.zeros_like(dqt_acc)

    def backward_tile(i, kv, diagonal):
        qs, ds = (qf[rows_of(i)], dof[rows_of(i)])
        half_score = nt(kv, qs)
        grad = nt(kv, ds)
        tanh = jnp.tanh(half_score)
        plus = 1.0 + tanh
        weight = half_score * plus
        slope = grad * (plus + weight * (1.0 - tanh))
        if diagonal:
            keep = tile_row <= tile_col
            weight = jnp.where(keep, weight, 0.0)
            slope = jnp.where(keep, slope, 0.0)
        slope = slope.astype(BF16)
        dqt_acc[i] += tn(kv[:, :64], slope)
        return nn(slope, qs) + nn(weight.astype(BF16), ds)

    to_core.wait_recv()
    to_x = []
    for d in range(1, NX):
        xx = (x + d) % NX
        x_send[d] = (term[core, xx] + core_got[xx].astype(F32)).astype(BF16)
        copy = remote(
            x_send.at[d], x_got.at[d], x_ssem.at[d], x_rsem.at[d],
            device(y_lo, z, y_hi, xx, core),
        )
        copy.start()
        to_x.append(copy)
    x_own[...] = term[core, x] + core_got[x].astype(F32)

    def down_copy(s):
        return remote(down_send.at[s], down_got.at[h], down_ss.at[s], down_rs.at[h], (g, s))

    def down_arrival(t):
        return remote(
            down_send.at[t], down_got.at[t], down_ss.at[t], down_rs.at[t], (g, HALF + t)
        )

    @pl.when(upper)
    def _():
        up_acc[...] = jnp.zeros_like(up_acc)

        @pl.loop(0, 4)
        def _(n):
            j = n // 2
            up_acc[rows_of(j)] += backward_tile(n % 2, upper_kv(j), False)

        for s in range(HALF):
            down_send[s] = up_acc[s * 128:(s + 1) * 128].astype(BF16)
            down_copy(s).start()

    for d in range(1, NX):
        to_x[d - 1].wait_recv()
        x_own[...] += x_got[d].astype(F32)
    for hi in range(2):
        for lo in range(NYL):
            piece = x_own[hi, lo * PIECE:(lo + 1) * PIECE]
            y_own[hi * NYL + lo] = piece
            y_send[hi * NYL + lo] = piece.astype(BF16)
    to_y = []
    for d in range(1, 2 * NYL):
        to = (y + d) % (2 * NYL)
        copy = remote(
            y_send.at[to], y_got.at[d], y_ssem.at[d], y_rsem.at[d],
            device(to % NYL, z, to // NYL, x, core),
        )
        copy.start()
        to_y.append(copy)

    @pl.loop(0, 2)
    def _(i):
        dkv_acc[rows_of(i)] += backward_tile(i, local_kv(i), True)

    dkv_acc[0:TILE] += backward_tile(1, local_kv(0), False)

    for s in range(HALF):
        i, at = (s // 4, (s % 4) * 128)
        back_send[s, 0:64] = (dqt_acc[i, :, at:at + 128] * 0.0625).astype(BF16)
        back_send[s, 64:192] = dkv_acc[s * 128:(s + 1) * 128].astype(BF16)
    back_got[h] = back_send[h]
    to_back = to_half(back_send, back_got, back_ss, back_rs)
    for copy in to_back:
        copy.start()

    total = y_own[y]
    for d in range(1, 2 * NYL):
        to_y[d - 1].wait_recv()
        total = total + y_got[d].astype(F32)
    z_all[z] = total.astype(BF16)
    to_z = []
    for d in range(1, NZ):
        copy = remote(
            z_all.at[z], z_all.at[z], z_ssem.at[d], z_rsem.at[d],
            device(y_lo, (z + d) % NZ, y_hi, x, core),
        )
        copy.start()
        to_z.append(copy)

    from_half(back_send, back_got, back_ss, back_rs)
    for p in range(HALF // 2):
        cols = slice(p * 128, (p + 1) * 128)
        pair = jnp.concatenate(
            [back_got[2 * p, 0:64].astype(F32), back_got[2 * p + 1, 0:64].astype(F32)], axis=0
        )
        gq_ref[:, cols] = pair.T.astype(BF16)

    for d in range(1, NZ):
        remote(
            z_all.at[z], z_all.at[(z + NZ - d) % NZ], z_ssem.at[d], z_rsem.at[d],
            device(y_lo, (z + d) % NZ, y_hi, x, core),
        ).wait_recv()
    total = z_all[0].astype(F32)
    for zz in range(1, NZ):
        total = total + z_all[zz].astype(F32)
    gathered[y_lo] = total
    to_g = []
    for d in range(1, NYL):
        copy = remote(
            gathered.at[y_lo], gathered.at[y_lo], g_ssem.at[d], g_rsem.at[d],
            device((y_lo + d) % NYL, z, y_hi, x, core),
        )
        copy.start()
        to_g.append(copy)

    @pl.when(lower)
    def _():
        for t in range(HALF):
            down_arrival(t).wait_recv()

    for p in range(HALF // 2):
        cols = slice(p * 128, (p + 1) * 128)
        heads = []
        for t in (2 * p, 2 * p + 1):
            mine = back_got[t, 64:192].astype(F32)
            far = jnp.where(lower, down_got[t].astype(F32), 0.0)
            heads.append(mine + far)
        kk, vv = join_heads(*heads)
        gk_ref[:, cols] = kk.astype(BF16)
        gv_ref[:, cols] = vv.astype(BF16)

    for d in range(1, NYL):
        remote(
            gathered.at[y_lo], gathered.at[(y_lo + NYL - d) % NYL], g_ssem.at[d], g_rsem.at[d],
            device((y_lo + d) % NYL, z, y_hi, x, core),
        ).wait_recv()
    gw_ref[...] = gathered[...].reshape(64, 512).T

    for copy in to_in + to_att + to_do + to_back + [to_core] + to_x + to_y + to_z + to_g:
        copy.wait_send()

    @pl.when(lower)
    def _():
        for t in range(HALF):
            up_copy(t).wait_send()

    @pl.when(upper)
    def _():
        for s in range(HALF):
            down_copy(s).wait_send()


def shards(query, key, value, gate_u, out_grad, lengths, norm_gain, out_weight):
    dma = pltpu.SemaphoreType.DMA
    vmem = pltpu.VMEM
    whole = pl.BlockSpec(memory_space=vmem)
    rows = query.shape[0]
    return pl.pallas_call(
        layer_kernel,
        out_shape=(
            jax.ShapeDtypeStruct((rows, 1024), BF16),
            jax.ShapeDtypeStruct((rows, 512), BF16),
            jax.ShapeDtypeStruct((rows, 512), BF16),
            jax.ShapeDtypeStruct((rows, 512), BF16),
            jax.ShapeDtypeStruct((rows, 512), BF16),
            jax.ShapeDtypeStruct((512, 64), F32),
        ),
        in_specs=[whole] * 5 + [pl.BlockSpec(memory_space=pltpu.SMEM)] + [whole] * 2,
        out_specs=(whole,) * 6,
        scratch_shapes=[
            vmem((HALF, 192, 128), BF16),
            vmem((HALF, 192, 128), BF16),
            vmem((HALF, 128, 128), BF16),
            vmem((1024, 128), BF16),
            vmem((1024, 128), BF16),
            vmem((1024, 128), F32),
            vmem((HALF, 64, 128), BF16),
            vmem((HALF, 64, 128), BF16),
            vmem((HALF, 64, 128), BF16),
            vmem((HALF, 64, 128), BF16),
            vmem((1024, 128), F32),
            vmem((2, 64, TILE), F32),
            vmem((1024, 128), F32),
            vmem((HALF, 192, 128), BF16),
            vmem((HALF, 192, 128), BF16),
            vmem((HALF, 128, 128), BF16),
            vmem((HALF, 128, 128), BF16),
            vmem((ROWS, 512), F32),
            vmem((ROWS, 512), F32),
            vmem((ROWS, 512), BF16),
            vmem((2, NX, 2, 64, 512), F32),
            vmem((2, NX, 2, 64, 512), BF16),
            vmem((NX, 2, 64, 512), BF16),
            vmem((2, 64, 512), F32),
            vmem((NX, 2, 64, 512), BF16),
            vmem((NX, 2, 64, 512), BF16),
            vmem((2 * NYL, PIECE, 512), F32),
            vmem((2 * NYL, PIECE, 512), BF16),
            vmem((2 * NYL, PIECE, 512), BF16),
            vmem((NZ, PIECE, 512), BF16),
            vmem((NYL, PIECE, 512), F32),
        ]
        + [dma((HALF,))] * 12
        + [
            dma((2,)), dma((NX,)), dma((NX,)), dma((2 * NYL,)), dma((2 * NYL,)),
            dma((NZ,)), dma((NZ,)), dma((NYL,)), dma((NYL,)),
        ],
        compiler_params=pltpu.CompilerParams(collective_id=0, has_side_effects=True),
    )(query, key, value, gate_u, out_grad, lengths, norm_gain.reshape(1, 512), out_weight)


def solution(mesh):
    split = P(("grp", "blk"), None)
    return jax.shard_map(
        shards,
        mesh=mesh,
        in_specs=(split,) * 5 + (P("grp"), P(), P()),
        out_specs=(split,) * 5 + (P(None, "blk"),),
        check_vma=False,
    )
```

```python
import jax
import jax.numpy as jnp
from jax import lax
from jax.experimental import pallas as pl
from jax.experimental.pallas import tpu as pltpu
from jax.sharding import PartitionSpec as P

MESH = pl.DeviceIdType.MESH
EPS = 1e-05
ZA = 4
ZB = 3
NZ = ZA * ZB
NYL = 4
NX = 4
HALF = 8
ROWS = 128
TILE = 512
F32 = jnp.float32
BF16 = jnp.bfloat16


def where_am_i():
    g, b = (lax.axis_index("grp"), lax.axis_index("blk"))
    return (g // NZ, g % NZ, b // 8, (b // 2) % NX, b % 2)


def device(y_lo, z, y_hi, x, core):
    return (y_lo * NZ + z, (y_hi * NX + x) * 2 + core)


def remote(src, dst, send_sem, recv_sem, target):
    return pltpu.make_async_remote_copy(
        src_ref=src, dst_ref=dst, send_sem=send_sem, recv_sem=recv_sem,
        device_id=target, device_id_type=MESH,
    )


def swap(part):
    return pltpu.roll(part.astype(F32), 64, 1)


def low_lanes(rows):
    return lax.broadcasted_iota(jnp.int32, (rows, 128), 1) < 64


def fold_rows(block, odd):
    low = low_lanes(64)
    top, bottom = (block[:64], block[64:])
    if odd:
        return jnp.where(low, swap(top), bottom.astype(F32))
    return jnp.where(low, top.astype(F32), swap(bottom))


def join_heads(even, odd):
    low = low_lanes(even.shape[0])
    return (jnp.where(low, even, swap(odd)), jnp.where(low, swap(even), odd))


def nt(left, right):
    return lax.dot_general(left, right, (((1,), (1,)), ((), ())), preferred_element_type=F32)


def tn(left, right):
    return lax.dot_general(left, right, (((0,), (0,)), ((), ())), preferred_element_type=F32)


def nn(left, right):
    return jnp.dot(left, right, preferred_element_type=F32)


def symmetric_partners(me):
    y_lo, z, y_hi, x, core = me
    mine = (y_hi * NX + x) * 2 + core
    y = y_hi * NYL + y_lo
    found = [(y_lo * NZ + z, (mine + d) % 16) for d in range(1, 16)]
    for d in range(1, 2 * NYL):
        if d != NYL:
            to = (y + d) % (2 * NYL)
            found.append(device(to % NYL, z, to // NYL, x, core))
    for d in range(1, ZA):
        found.append(device(y_lo, near_z(z, d), y_hi, x, core))
    for d in range(1, ZB):
        found.append(device(y_lo, far_z(z, d), y_hi, x, core))
    for d in range(1, NYL):
        for cc in range(2):
            found.append(device((y_lo + d) % NYL, z, y_hi, y_lo, cc))
    return found


def near_z(z, d):
    return z // ZA * ZA + (z % ZA + d) % ZA


def far_z(z, d):
    return (z // ZA + d) % ZB * ZA + z % ZA


def layer_kernel(
    q_hbm, k_hbm, v_hbm, gate_hbm, cot_hbm, length_hbm, gain_hbm, weight_hbm,
    out_ref, gq_ref, gk_ref, gv_ref, gg_ref, gw_ref,
    q_ref, k_ref, v_ref, gate_ref, length_ref, gain_ref, weight_ref,
    in_send, in_got, side_send, side_got, up_got, cot_all, gain_cols,
    qf, dot_ref, att_acc, stat_send, stat_got, mix_send, mix_got,
    dkv_acc, dqt_acc, up_acc, back_send, back_got, down_send, down_got,
    y_own, y_send, y_got, near_all, far_all, fin_send, fin_got, fin_turned,
    load, in_ss, in_rs, side_ss, side_rs, up_ss, up_rs, cot_ss, cot_rs, rel_ss, rel_rs,
    stat_ss, stat_rs, mix_ss, mix_rs, back_ss, back_rs, down_ss, down_rs,
    y_ss, y_rs, near_ss, near_rs, far_ss, far_rs, fin_ss, fin_rs,
):
    me = where_am_i()
    y_lo, z, y_hi, x, core = me
    g = y_lo * NZ + z
    y = y_hi * NYL + y_lo
    h = x * 2 + core
    base = y_hi * HALF
    upper = y_hi == 1
    lower = y_hi == 0

    loads = [
        pltpu.make_async_copy(k_hbm, k_ref, load.at[0]),
        pltpu.make_async_copy(v_hbm, v_ref, load.at[1]),
        pltpu.make_async_copy(q_hbm, q_ref, load.at[2]),
        pltpu.make_async_copy(gate_hbm, gate_ref, load.at[3]),
        pltpu.make_async_copy(cot_hbm, cot_all.at[h], load.at[4]),
        pltpu.make_async_copy(weight_hbm, weight_ref, load.at[5]),
        pltpu.make_async_copy(gain_hbm, gain_ref, load.at[6]),
        pltpu.make_async_copy(length_hbm, length_ref, load.at[7]),
    ]
    for copy in loads:
        copy.start()

    def far_sources():
        return [device(x, z, y_hi, xx, cc) for xx in range(NX) for cc in range(2)]

    barrier = pltpu.get_barrier_semaphore()
    partners = symmetric_partners(me)
    for target in partners:
        pl.semaphore_signal(barrier, inc=1, device_id=target, device_id_type=MESH)

    @pl.when(x != y_lo)
    def _():
        for target in far_sources():
            pl.semaphore_signal(barrier, inc=1, device_id=target, device_id_type=MESH)

    for copy in loads[:3]:
        copy.wait()
    low128 = low_lanes(128)
    for t in range(HALF):
        cols = slice((t // 2) * 128, (t // 2 + 1) * 128)
        kk, vv = (k_ref[:, cols], v_ref[:, cols])
        if t % 2:
            pair = jnp.where(low128, swap(kk), vv.astype(F32))
        else:
            pair = jnp.where(low128, kk.astype(F32), swap(vv))
        in_send[t, 64:192] = pair.astype(BF16)
        in_send[t, 0:64] = (fold_rows(q_ref[:, cols], t % 2) * 0.0625).astype(BF16)
    in_got[h] = in_send[h]

    @pl.when(x != y_lo)
    def _():
        pl.semaphore_wait(barrier, len(partners) + HALF)

    @pl.when(x == y_lo)
    def _():
        pl.semaphore_wait(barrier, len(partners))

    def up_copy(t):
        return remote(
            in_send.at[t, pl.ds(64, 128)], up_got.at[h], up_ss.at[t], up_rs.at[h], (g, HALF + t)
        )

    def up_arrival(s):
        return remote(
            in_send.at[s, pl.ds(64, 128)], up_got.at[s], up_ss.at[s], up_rs.at[s], (g, s)
        )

    @pl.when(lower)
    def _():
        for t in range(HALF):
            up_copy(t).start()

    def to_half(send, got, ssem, rsem):
        copies = []
        for d in range(1, HALF):
            t = (h + d) % HALF
            copies.append(remote(send.at[t], got.at[h], ssem.at[d], rsem.at[d], (g, base + t)))
        for copy in copies:
            copy.start()
        return copies

    def from_half(send, got, ssem, rsem):
        for d in range(1, HALF):
            t = (h + d) % HALF
            s = (h + HALF - d) % HALF
            remote(send.at[t], got.at[s], ssem.at[d], rsem.at[d], (g, base + t)).wait_recv()

    sent = to_half(in_send, in_got, in_ss, in_rs)

    for copy in loads[3:7]:
        copy.wait()
    for p in range(HALF // 2):
        cols = slice(p * 128, (p + 1) * 128)
        turned = gate_ref[:, cols].astype(F32).T.astype(BF16)
        side_send[2 * p, 0:64] = turned[:64]
        side_send[2 * p + 1, 0:64] = turned[64:]
        spread = jnp.broadcast_to(gain_ref[:, cols], (128, 128)).T
        gain_cols[2 * p] = spread[:64]
        gain_cols[2 * p + 1] = spread[64:]
        grads = nt(weight_ref[cols], cot_all[h]).astype(BF16)
        side_send[2 * p, 64:128] = grads[:64]
        side_send[2 * p + 1, 64:128] = grads[64:]
    side_got[h] = side_send[h]
    sent += to_half(side_send, side_got, side_ss, side_rs)

    sister = (g, base + h + 1 - 2 * core)
    for d in range(1, NX):
        copy = remote(
            cot_all.at[h], cot_all.at[h], cot_ss.at[d], cot_rs.at[d],
            device(y_lo, z, y_hi, (x + d) % NX, core),
        )
        copy.start()
        sent.append(copy)

    def relay(d):
        slot = (x + NX - d) % NX * 2 + core
        return remote(cot_all.at[slot], cot_all.at[slot], rel_ss.at[d], rel_rs.at[d], sister)

    def relay_arrival(d):
        slot = (x + NX - d) % NX * 2 + 1 - core
        return remote(cot_all.at[slot], cot_all.at[slot], rel_ss.at[d], rel_rs.at[d], sister)

    first = relay(0)
    first.start()
    sent.append(first)

    from_half(in_send, in_got, in_ss, in_rs)
    low64 = low_lanes(64)
    for s in range(HALF):
        folded = in_got[s, 0:64].astype(F32)
        qf[s * 128:s * 128 + 64] = jnp.where(low64, folded, 0.0).astype(BF16)
        qf[s * 128 + 64:s * 128 + 128] = jnp.where(low64, swap(folded), 0.0).astype(BF16)
    att_acc[...] = jnp.zeros_like(att_acc)
    dkv_acc[...] = jnp.zeros_like(dkv_acc)
    dqt_acc[...] = jnp.zeros_like(dqt_acc)

    def local_kv(j):
        return in_got[pl.ds(j * 4, 4), 64:192].reshape(TILE, 128)

    def upper_kv(j):
        return up_got[pl.ds(j * 4, 4)].reshape(TILE, 128)

    def rows_of(i):
        return pl.ds(pl.multiple_of(i * TILE, TILE), TILE)

    tile_row = lax.broadcasted_iota(jnp.int32, (TILE, TILE), 0)
    tile_col = lax.broadcasted_iota(jnp.int32, (TILE, TILE), 1)

    def forward_tile(i, kv, diagonal):
        half_score = nt(kv, qf[rows_of(i)])
        weight = half_score + half_score * jnp.tanh(half_score)
        if diagonal:
            weight = jnp.where(tile_row <= tile_col, weight, 0.0)
        att_acc[i] += tn(kv[:, 64:], weight.astype(BF16))

    @pl.loop(0, 2)
    def _(i):
        forward_tile(i, local_kv(i), True)

    forward_tile(1, local_kv(0), False)
    from_half(side_send, side_got, side_ss, side_rs)
    loads[7].wait()
    gates = jnp.concatenate([side_got[s, 0:64] for s in range(HALF)], axis=1).astype(F32)
    grads = jnp.concatenate([side_got[s, 64:128] for s in range(HALF)], axis=1).astype(F32)
    gain = gain_cols[h][:, 0:1]
    normed_grad = grads * gates * gain
    position = base * ROWS + lax.broadcasted_iota(jnp.int32, (1, HALF * ROWS), 1)
    alive = position < length_ref[0]

    @pl.when(upper)
    def _():
        for j in range(2):
            for s in range(4):
                up_arrival(4 * j + s).wait_recv()

            @pl.loop(0, 2)
            def _(i):
                forward_tile(i, upper_kv(j), False)

    attended = jnp.where(alive, jnp.concatenate([att_acc[0], att_acc[1]], axis=1), 0.0)
    mean_mine = jnp.sum(attended, axis=0, keepdims=True) * (1.0 / 64)
    centre = attended - mean_mine
    stats = (
        mean_mine,
        jnp.sum(centre * centre, axis=0, keepdims=True),
        jnp.sum(normed_grad, axis=0, keepdims=True),
        jnp.sum(normed_grad * centre, axis=0, keepdims=True),
    )
    for n, stat in enumerate(stats):
        stat_send[n:n + 1] = stat[:, :TILE]
        stat_send[n + 4:n + 5] = stat[:, TILE:]
    stat_got[h] = stat_send[...]
    for d in range(1, HALF):
        t = (h + d) % HALF
        copy = remote(stat_send, stat_got.at[h], stat_ss.at[d], stat_rs.at[d], (g, base + t))
        copy.start()
        sent.append(copy)
    for d in range(1, NX):
        slot = (x + NX - d) % NX * 2 + core
        remote(
            cot_all.at[h], cot_all.at[slot], cot_ss.at[d], cot_rs.at[d],
            device(y_lo, z, y_hi, (x + d) % NX, core),
        ).wait_recv()
        copy = relay(d)
        copy.start()
        sent.append(copy)
    for d in range(1, HALF):
        t = (h + d) % HALF
        s = (h + HALF - d) % HALF
        remote(
            stat_send, stat_got.at[s], stat_ss.at[d], stat_rs.at[d], (g, base + t)
        ).wait_recv()

    def stat_rows(n):
        return [
            jnp.concatenate([stat_got[s, n:n + 1], stat_got[s, n + 4:n + 5]], axis=1)
            for s in range(HALF)
        ]

    means, squares, sums, products = (stat_rows(n) for n in range(4))
    mean = sum(means) * (1.0 / HALF)
    square = sum(squares)
    grad_sum = sum(sums)
    product = sum(products)
    for s in range(HALF):
        off = means[s] - mean
        square = square + 64.0 * (off * off)
        product = product + off * sums[s]
    inv_std = lax.rsqrt(square * (1.0 / 512) + EPS)
    grad_mean = grad_sum * (1.0 / 512)
    product_mean = inv_std * product * (1.0 / 512)
    normed = (attended - mean) * inv_std
    scaled = normed * gain
    mixed = (scaled * gates).astype(BF16)
    grad_gate = (grads * scaled).astype(BF16)
    attended_grad = inv_std * (normed_grad - grad_mean - normed * product_mean)
    attended_grad = jnp.where(alive, attended_grad, 0.0).astype(BF16)
    dot_ref[0:64] = jnp.zeros_like(attended_grad)
    dot_ref[64:128] = attended_grad
    for s in range(HALF):
        mix_send[s, 0:64] = mixed[:, s * 128:(s + 1) * 128]
        mix_send[s, 64:128] = grad_gate[:, s * 128:(s + 1) * 128]
    mix_got[h] = mix_send[h]
    sent += to_half(mix_send, mix_got, mix_ss, mix_rs)

    for d in range(NX):
        relay_arrival(d).wait_recv()
    for n in range(2 * NYL):
        part = nn(mixed, cot_all[:, :, n * 128:(n + 1) * 128].reshape(HALF * ROWS, 128))
        y_own[n] = part
        y_send[n] = part.astype(BF16)
    to_y = []
    for d in range(1, 2 * NYL):
        to = (y + d) % (2 * NYL)
        copy = remote(
            y_send.at[to], y_got.at[d], y_ss.at[d], y_rs.at[d],
            device(to % NYL, z, to // NYL, x, core),
        )
        copy.start()
        to_y.append(copy)

    def columns_of(i):
        return pl.ds(pl.multiple_of(i * TILE, TILE), TILE)

    def backward_tile(i, kv, diagonal):
        qs, dots = (qf[rows_of(i)], dot_ref[:, columns_of(i)])
        half_score = nt(kv, qs)
        grad = nn(kv, dots)
        tanh = jnp.tanh(half_score)
        plus = 1.0 + tanh
        weight = half_score * plus
        slope = grad * (plus + weight * (1.0 - tanh))
        if diagonal:
            keep = tile_row <= tile_col
            weight = jnp.where(keep, weight, 0.0)
            slope = jnp.where(keep, slope, 0.0)
        slope = slope.astype(BF16)
        dqt_acc[i] += tn(kv[:, :64], slope)
        return nn(slope, qs) + nt(weight.astype(BF16), dots)

    def down_copy(s):
        return remote(down_send.at[s], down_got.at[h], down_ss.at[s], down_rs.at[h], (g, s))

    def down_arrival(t):
        return remote(
            down_send.at[t], down_got.at[t], down_ss.at[t], down_rs.at[t], (g, HALF + t)
        )

    @pl.when(upper)
    def _():
        for j in range(2):
            up_acc[...] = jnp.zeros_like(up_acc)

            @pl.loop(0, 2)
            def _(i):
                up_acc[...] += backward_tile(i, upper_kv(j), False)

            for s in range(4):
                down_send[4 * j + s] = up_acc[s * 128:(s + 1) * 128].astype(BF16)
                down_copy(4 * j + s).start()

    total = y_own[y]
    for d in range(1, 2 * NYL):
        to_y[d - 1].wait_recv()
        total = total + y_got[d].astype(F32)
    near_all[z % ZA] = total.astype(BF16)
    for d in range(1, ZA):
        copy = remote(
            near_all.at[z % ZA], near_all.at[z % ZA], near_ss.at[d], near_rs.at[d],
            device(y_lo, near_z(z, d), y_hi, x, core),
        )
        copy.start()
        sent.append(copy)

    @pl.loop(0, 2)
    def _(i):
        dkv_acc[rows_of(i)] += backward_tile(i, local_kv(i), True)

    dkv_acc[0:TILE] += backward_tile(1, local_kv(0), False)

    for s in range(HALF):
        i, at = (s // 4, (s % 4) * 128)
        back_send[s, 0:64] = (dqt_acc[i, :, at:at + 128] * 0.0625).astype(BF16)
        back_send[s, 64:192] = dkv_acc[s * 128:(s + 1) * 128].astype(BF16)
    back_got[h] = back_send[h]
    sent += to_half(back_send, back_got, back_ss, back_rs)

    for d in range(1, ZA):
        remote(
            near_all.at[z % ZA], near_all.at[(z % ZA + ZA - d) % ZA], near_ss.at[d], near_rs.at[d],
            device(y_lo, near_z(z, d), y_hi, x, core),
        ).wait_recv()
    total = near_all[0].astype(F32)
    for n in range(1, ZA):
        total = total + near_all[n].astype(F32)
    far_all[z // ZA] = total.astype(BF16)
    for d in range(1, ZB):
        copy = remote(
            far_all.at[z // ZA], far_all.at[z // ZA], far_ss.at[d], far_rs.at[d],
            device(y_lo, far_z(z, d), y_hi, x, core),
        )
        copy.start()
        sent.append(copy)

    from_half(mix_send, mix_got, mix_ss, mix_rs)
    whole = jnp.concatenate([mix_got[t, 0:64] for t in range(HALF)], axis=0)
    out_ref[...] = tn(whole, weight_ref[...]).astype(BF16)
    for p in range(HALF // 2):
        pair = jnp.concatenate(
            [mix_got[2 * p, 64:128].astype(F32), mix_got[2 * p + 1, 64:128].astype(F32)], axis=0
        )
        gg_ref[:, p * 128:(p + 1) * 128] = pair.T.astype(BF16)

    for d in range(1, ZB):
        remote(
            far_all.at[z // ZA], far_all.at[(z // ZA + ZB - d) % ZB], far_ss.at[d], far_rs.at[d],
            device(y_lo, far_z(z, d), y_hi, x, core),
        ).wait_recv()
    total = far_all[0].astype(F32)
    for n in range(1, ZB):
        total = total + far_all[n].astype(F32)
    fin_send[...] = total.astype(BF16)

    def fin_copy(lo, cc):
        return remote(
            fin_send, fin_got.at[h], fin_ss.at[lo * 2 + cc], fin_rs.at[h],
            device(lo, z, y_hi, y_lo, cc),
        )

    def not_me(lo, cc):
        return (x != y_lo) | (lo != y_lo) | (cc != core)

    for lo in range(NYL):
        for cc in range(2):

            @pl.when(not_me(lo, cc))
            def _():
                fin_copy(lo, cc).start()

    @pl.when(x == y_lo)
    def _():
        fin_got[h] = fin_send[...]

    from_half(back_send, back_got, back_ss, back_rs)
    for p in range(HALF // 2):
        pair = jnp.concatenate(
            [back_got[2 * p, 0:64].astype(F32), back_got[2 * p + 1, 0:64].astype(F32)], axis=0
        )
        gq_ref[:, p * 128:(p + 1) * 128] = pair.T.astype(BF16)

    @pl.when(lower)
    def _():
        for t in range(HALF):
            down_arrival(t).wait_recv()

    for p in range(HALF // 2):
        cols = slice(p * 128, (p + 1) * 128)
        heads = []
        for t in (2 * p, 2 * p + 1):
            mine = back_got[t, 64:192].astype(F32)
            far = jnp.where(lower, down_got[t].astype(F32), 0.0)
            heads.append(mine + far)
        kk, vv = join_heads(*heads)
        gk_ref[:, cols] = kk.astype(BF16)
        gv_ref[:, cols] = vv.astype(BF16)

    for xx in range(NX):
        for cc in range(2):
            t = xx * 2 + cc

            @pl.when((x != y_lo) | (h != t))
            def _():
                remote(
                    fin_send, fin_got.at[t], fin_ss.at[t], fin_rs.at[t],
                    device(x, z, y_hi, xx, cc),
                ).wait_recv()

    for p in range(HALF // 2):
        pair = jnp.concatenate(
            [fin_got[2 * p].astype(F32), fin_got[2 * p + 1].astype(F32)], axis=0
        )
        fin_turned[:, p * 128:(p + 1) * 128] = pair.T
    gw_ref[...] = fin_turned[pl.ds(pl.multiple_of(core * 64, 64), 64)]

    for copy in sent + to_y:
        copy.wait_send()
    for lo in range(NYL):
        for cc in range(2):

            @pl.when(not_me(lo, cc))
            def _():
                fin_copy(lo, cc).wait_send()

    @pl.when(lower)
    def _():
        for t in range(HALF):
            up_copy(t).wait_send()

    @pl.when(upper)
    def _():
        for s in range(HALF):
            down_copy(s).wait_send()


def shards(query, key, value, gate_u, out_grad, lengths, norm_gain, out_weight):
    dma = pltpu.SemaphoreType.DMA
    vmem = pltpu.VMEM
    rows = query.shape[0]
    outs = [((rows, 1024), BF16)] + [((rows, 512), BF16)] * 4 + [((64, 512), F32)]
    results = pl.pallas_call(
        layer_kernel,
        out_shape=tuple(vmem(*out) for out in outs),
        in_specs=[pl.BlockSpec(memory_space=pl.ANY)] * 8,
        out_specs=(pl.BlockSpec(memory_space=vmem),) * 6,
        scratch_shapes=[
            vmem((ROWS, 512), BF16),
            vmem((ROWS, 512), BF16),
            vmem((ROWS, 512), BF16),
            vmem((ROWS, 512), BF16),
            pltpu.SMEM((1,), jnp.int32),
            vmem((1, 512), F32),
            vmem((512, 1024), BF16),
            vmem((HALF, 192, 128), BF16),
            vmem((HALF, 192, 128), BF16),
            vmem((HALF, 128, 128), BF16),
            vmem((HALF, 128, 128), BF16),
            vmem((HALF, 128, 128), BF16),
            vmem((HALF, ROWS, 1024), BF16),
            vmem((HALF, 64, 128), F32),
            vmem((1024, 128), BF16),
            vmem((128, 1024), BF16),
            vmem((2, 64, TILE), F32),
            vmem((8, TILE), F32),
            vmem((HALF, 8, TILE), F32),
            vmem((HALF, 128, 128), BF16),
            vmem((HALF, 128, 128), BF16),
            vmem((1024, 128), F32),
            vmem((2, 64, TILE), F32),
            vmem((TILE, 128), F32),
            vmem((HALF, 192, 128), BF16),
            vmem((HALF, 192, 128), BF16),
            vmem((HALF, 128, 128), BF16),
            vmem((HALF, 128, 128), BF16),
            vmem((2 * NYL, 64, 128), F32),
            vmem((2 * NYL, 64, 128), BF16),
            vmem((2 * NYL, 64, 128), BF16),
            vmem((ZA, 64, 128), BF16),
            vmem((ZB, 64, 128), BF16),
            vmem((64, 128), BF16),
            vmem((HALF, 64, 128), BF16),
            vmem((128, 512), F32),
        ]
        + [dma((HALF,))] * 27,
        compiler_params=pltpu.CompilerParams(collective_id=0, has_side_effects=True),
    )(query, key, value, gate_u, out_grad, lengths, norm_gain.reshape(1, 512), out_weight)
    anywhere = pl.BlockSpec(memory_space=pl.ANY)
    results = pl.pallas_call(
        store_kernel,
        out_shape=tuple(jax.ShapeDtypeStruct(*out) for out in outs),
        in_specs=[pl.BlockSpec(memory_space=vmem)] * 6,
        out_specs=(anywhere,) * 6,
        scratch_shapes=[dma((6,))],
    )(*[pltpu.with_memory_space_constraint(one, vmem) for one in results])
    return (*results[:5], results[5].T)


def store_kernel(*refs):
    sources, targets, sems = (refs[:6], refs[6:12], refs[12])
    copies = [
        pltpu.make_async_copy(source, target, sems.at[n])
        for n, (source, target) in enumerate(zip(sources, targets))
    ]
    for copy in copies:
        copy.start()
    for copy in copies:
        copy.wait()


def solution(mesh):
    split = P(("grp", "blk"), None)
    return jax.shard_map(
        shards,
        mesh=mesh,
        in_specs=(split,) * 5 + (P("grp"), P(), P()),
        out_specs=(split,) * 5 + (P(None, "blk"),),
        check_vma=False,
    )
```

```python
import jax
import jax.numpy as jnp
from jax import lax
from jax.experimental import pallas as pl
from jax.experimental.pallas import tpu as pltpu
from jax.sharding import PartitionSpec as P

MESH = pl.DeviceIdType.MESH
EPS = 1e-05
ZA = 4
ZB = 3
NZ = ZA * ZB
NYL = 4
NX = 4
HALF = 8
ROWS = 128
TILE = 512
F32 = jnp.float32
BF16 = jnp.bfloat16


def where_am_i():
    g, b = (lax.axis_index("grp"), lax.axis_index("blk"))
    return (g // NZ, g % NZ, b // 8, (b // 2) % NX, b % 2)


def device(y_lo, z, y_hi, x, core):
    return (y_lo * NZ + z, (y_hi * NX + x) * 2 + core)


def remote(src, dst, send_sem, recv_sem, target):
    return pltpu.make_async_remote_copy(
        src_ref=src, dst_ref=dst, send_sem=send_sem, recv_sem=recv_sem,
        device_id=target, device_id_type=MESH,
    )


def swap(part):
    return pltpu.roll(part.astype(F32), 64, 1)


def low_lanes(rows):
    return lax.broadcasted_iota(jnp.int32, (rows, 128), 1) < 64


def fold_rows(block, odd):
    low = low_lanes(64)
    top, bottom = (block[:64], block[64:])
    if odd:
        return jnp.where(low, swap(top), bottom.astype(F32))
    return jnp.where(low, top.astype(F32), swap(bottom))


def join_heads(even, odd):
    low = low_lanes(even.shape[0])
    return (jnp.where(low, even, swap(odd)), jnp.where(low, swap(even), odd))


def nt(left, right):
    return lax.dot_general(left, right, (((1,), (1,)), ((), ())), preferred_element_type=F32)


def tn(left, right):
    return lax.dot_general(left, right, (((0,), (0,)), ((), ())), preferred_element_type=F32)


def nn(left, right):
    return jnp.dot(left, right, preferred_element_type=F32)


def symmetric_partners(me):
    y_lo, z, y_hi, x, core = me
    mine = (y_hi * NX + x) * 2 + core
    y = y_hi * NYL + y_lo
    found = [(y_lo * NZ + z, (mine + d) % 16) for d in range(1, 16)]
    for d in range(1, 2 * NYL):
        if d != NYL:
            to = (y + d) % (2 * NYL)
            found.append(device(to % NYL, z, to // NYL, x, core))
    for d in range(1, ZA):
        found.append(device(y_lo, near_z(z, d), y_hi, x, core))
    for d in range(1, ZB):
        found.append(device(y_lo, far_z(z, d), y_hi, x, core))
    for d in range(1, NYL):
        for cc in range(2):
            found.append(device((y_lo + d) % NYL, z, y_hi, y_lo, cc))
    return found


def near_z(z, d):
    return z // ZA * ZA + (z % ZA + d) % ZA


def far_z(z, d):
    return (z // ZA + d) % ZB * ZA + z % ZA


def layer_kernel(
    q_hbm, k_hbm, v_hbm, gate_hbm, cot_hbm, length_hbm, gain_hbm, weight_hbm,
    out_ref, gq_ref, gk_ref, gv_ref, gg_ref, gw_ref,
    q_ref, k_ref, v_ref, gate_ref, length_ref, gain_ref, weight_ref,
    in_send, in_got, side_send, side_got, up_got, cot_all, gain_cols,
    qf, dot_ref, att_acc, stat_send, stat_got, mix_send, mix_got,
    dkv_acc, dqt_acc, up_acc, back_send, back_got, down_send, down_got,
    y_own, y_send, y_got, near_all, far_all, fin_send, fin_got, fin_turned,
    load, in_ss, in_rs, side_ss, side_rs, up_ss, up_rs, cot_ss, cot_rs, rel_ss, rel_rs,
    stat_ss, stat_rs, mix_ss, mix_rs, back_ss, back_rs, down_ss, down_rs,
    y_ss, y_rs, near_ss, near_rs, far_ss, far_rs, fin_ss, fin_rs,
):
    me = where_am_i()
    y_lo, z, y_hi, x, core = me
    g = y_lo * NZ + z
    y = y_hi * NYL + y_lo
    h = x * 2 + core
    base = y_hi * HALF
    upper = y_hi == 1
    lower = y_hi == 0

    loads = [
        pltpu.make_async_copy(k_hbm, k_ref, load.at[0]),
        pltpu.make_async_copy(v_hbm, v_ref, load.at[1]),
        pltpu.make_async_copy(q_hbm, q_ref, load.at[2]),
        pltpu.make_async_copy(gate_hbm, gate_ref, load.at[3]),
        pltpu.make_async_copy(cot_hbm, cot_all.at[h], load.at[4]),
        pltpu.make_async_copy(weight_hbm, weight_ref, load.at[5]),
        pltpu.make_async_copy(gain_hbm, gain_ref, load.at[6]),
        pltpu.make_async_copy(length_hbm, length_ref, load.at[7]),
    ]
    for copy in loads:
        copy.start()

    def far_sources():
        return [device(x, z, y_hi, xx, cc) for xx in range(NX) for cc in range(2)]

    barrier = pltpu.get_barrier_semaphore()
    partners = symmetric_partners(me)
    for target in partners:
        pl.semaphore_signal(barrier, inc=1, device_id=target, device_id_type=MESH)

    @pl.when(x != y_lo)
    def _():
        for target in far_sources():
            pl.semaphore_signal(barrier, inc=1, device_id=target, device_id_type=MESH)

    for copy in loads[:3]:
        copy.wait()
    low128 = low_lanes(128)
    for t in range(HALF):
        cols = slice((t // 2) * 128, (t // 2 + 1) * 128)
        kk, vv = (k_ref[:, cols], v_ref[:, cols])
        if t % 2:
            pair = jnp.where(low128, swap(kk), vv.astype(F32))
        else:
            pair = jnp.where(low128, kk.astype(F32), swap(vv))
        in_send[t, 64:192] = pair.astype(BF16)
        in_send[t, 0:64] = (fold_rows(q_ref[:, cols], t % 2) * 0.0625).astype(BF16)
    in_got[h] = in_send[h]

    @pl.when(x != y_lo)
    def _():
        pl.semaphore_wait(barrier, len(partners) + HALF)

    @pl.when(x == y_lo)
    def _():
        pl.semaphore_wait(barrier, len(partners))

    def up_copy(t):
        return remote(
            in_send.at[t, pl.ds(64, 128)], up_got.at[h], up_ss.at[t], up_rs.at[h], (g, HALF + t)
        )

    def up_arrival(s):
        return remote(
            in_send.at[s, pl.ds(64, 128)], up_got.at[s], up_ss.at[s], up_rs.at[s], (g, s)
        )

    @pl.when(lower)
    def _():
        for t in range(HALF):
            up_copy(t).start()

    def to_half(send, got, ssem, rsem):
        copies = []
        for d in range(1, HALF):
            t = (h + d) % HALF
            copies.append(remote(send.at[t], got.at[h], ssem.at[d], rsem.at[d], (g, base + t)))
        for copy in copies:
            copy.start()
        return copies

    def from_half(send, got, ssem, rsem):
        for d in range(1, HALF):
            t = (h + d) % HALF
            s = (h + HALF - d) % HALF
            remote(send.at[t], got.at[s], ssem.at[d], rsem.at[d], (g, base + t)).wait_recv()

    sent = to_half(in_send, in_got, in_ss, in_rs)

    for copy in loads[3:7]:
        copy.wait()
    for p in range(HALF // 2):
        cols = slice(p * 128, (p + 1) * 128)
        turned = gate_ref[:, cols].astype(F32).T.astype(BF16)
        side_send[2 * p, 0:64] = turned[:64]
        side_send[2 * p + 1, 0:64] = turned[64:]
        spread = jnp.broadcast_to(gain_ref[:, cols], (128, 128)).T
        gain_cols[2 * p] = spread[:64]
        gain_cols[2 * p + 1] = spread[64:]
        grads = nt(weight_ref[cols], cot_all[h]).astype(BF16)
        side_send[2 * p, 64:128] = grads[:64]
        side_send[2 * p + 1, 64:128] = grads[64:]
    side_got[h] = side_send[h]
    sent += to_half(side_send, side_got, side_ss, side_rs)

    sister = (g, base + h + 1 - 2 * core)

    def slot_of(d):
        return (x + NX - d) % NX * 2 + core

    def to_chip(part, d, n):
        return remote(
            part, part, cot_ss.at[n], cot_rs.at[n], device(y_lo, z, y_hi, (x + d) % NX, core)
        )

    for d in (1, 3):
        copy = to_chip(cot_all.at[h], d, d)
        copy.start()
        sent.append(copy)

    def relay(d):
        slot = (x + NX - d) % NX * 2 + core
        return remote(cot_all.at[slot], cot_all.at[slot], rel_ss.at[d], rel_rs.at[d], sister)

    def relay_arrival(d):
        slot = (x + NX - d) % NX * 2 + 1 - core
        return remote(cot_all.at[slot], cot_all.at[slot], rel_ss.at[d], rel_rs.at[d], sister)

    first = relay(0)
    first.start()
    sent.append(first)

    from_half(in_send, in_got, in_ss, in_rs)
    low64 = low_lanes(64)
    for s in range(HALF):
        folded = in_got[s, 0:64].astype(F32)
        qf[s * 128:s * 128 + 64] = jnp.where(low64, folded, 0.0).astype(BF16)
        qf[s * 128 + 64:s * 128 + 128] = jnp.where(low64, swap(folded), 0.0).astype(BF16)
    att_acc[...] = jnp.zeros_like(att_acc)
    dkv_acc[...] = jnp.zeros_like(dkv_acc)
    dqt_acc[...] = jnp.zeros_like(dqt_acc)

    def local_kv(j):
        return in_got[pl.ds(j * 4, 4), 64:192].reshape(TILE, 128)

    def upper_kv(j):
        return up_got[pl.ds(j * 4, 4)].reshape(TILE, 128)

    def rows_of(i):
        return pl.ds(pl.multiple_of(i * TILE, TILE), TILE)

    tile_row = lax.broadcasted_iota(jnp.int32, (TILE, TILE), 0)
    tile_col = lax.broadcasted_iota(jnp.int32, (TILE, TILE), 1)

    def forward_tile(i, kv, diagonal):
        half_score = nt(kv, qf[rows_of(i)])
        weight = half_score + half_score * jnp.tanh(half_score)
        if diagonal:
            weight = jnp.where(tile_row <= tile_col, weight, 0.0)
        att_acc[i] += tn(kv[:, 64:], weight.astype(BF16))

    @pl.loop(0, 2)
    def _(i):
        forward_tile(i, local_kv(i), True)

    forward_tile(1, local_kv(0), False)
    to_chip(cot_all.at[slot_of(1)], 1, 1).wait_recv()
    to_chip(cot_all.at[slot_of(3)], 3, 3).wait_recv()
    for copy in (
        to_chip(cot_all.at[slot_of(1), pl.ds(0, 64)], 1, 4),
        to_chip(cot_all.at[slot_of(3), pl.ds(64, 64)], 3, 5),
        relay(1),
        relay(3),
    ):
        copy.start()
        sent.append(copy)
    from_half(side_send, side_got, side_ss, side_rs)
    loads[7].wait()
    gates = jnp.concatenate([side_got[s, 0:64] for s in range(HALF)], axis=1).astype(F32)
    grads = jnp.concatenate([side_got[s, 64:128] for s in range(HALF)], axis=1).astype(F32)
    gain = gain_cols[h][:, 0:1]
    normed_grad = grads * gates * gain
    position = base * ROWS + lax.broadcasted_iota(jnp.int32, (1, HALF * ROWS), 1)
    alive = position < length_ref[0]

    @pl.when(upper)
    def _():
        for j in range(2):
            for s in range(4):
                up_arrival(4 * j + s).wait_recv()

            @pl.loop(0, 2)
            def _(i):
                forward_tile(i, upper_kv(j), False)

    attended = jnp.where(alive, jnp.concatenate([att_acc[0], att_acc[1]], axis=1), 0.0)
    mean_mine = jnp.sum(attended, axis=0, keepdims=True) * (1.0 / 64)
    centre = attended - mean_mine
    stats = (
        mean_mine,
        jnp.sum(centre * centre, axis=0, keepdims=True),
        jnp.sum(normed_grad, axis=0, keepdims=True),
        jnp.sum(normed_grad * centre, axis=0, keepdims=True),
    )
    for n, stat in enumerate(stats):
        stat_send[n:n + 1] = stat[:, :TILE]
        stat_send[n + 4:n + 5] = stat[:, TILE:]
    stat_got[h] = stat_send[...]
    for d in range(1, HALF):
        t = (h + d) % HALF
        copy = remote(stat_send, stat_got.at[h], stat_ss.at[d], stat_rs.at[d], (g, base + t))
        copy.start()
        sent.append(copy)
    to_chip(cot_all.at[slot_of(2), pl.ds(0, 64)], 1, 4).wait_recv()
    to_chip(cot_all.at[slot_of(2), pl.ds(64, 64)], 3, 5).wait_recv()
    copy = relay(2)
    copy.start()
    sent.append(copy)
    for d in range(1, HALF):
        t = (h + d) % HALF
        s = (h + HALF - d) % HALF
        remote(
            stat_send, stat_got.at[s], stat_ss.at[d], stat_rs.at[d], (g, base + t)
        ).wait_recv()

    def stat_rows(n):
        return [
            jnp.concatenate([stat_got[s, n:n + 1], stat_got[s, n + 4:n + 5]], axis=1)
            for s in range(HALF)
        ]

    means, squares, sums, products = (stat_rows(n) for n in range(4))
    mean = sum(means) * (1.0 / HALF)
    square = sum(squares)
    grad_sum = sum(sums)
    product = sum(products)
    for s in range(HALF):
        off = means[s] - mean
        square = square + 64.0 * (off * off)
        product = product + off * sums[s]
    inv_std = lax.rsqrt(square * (1.0 / 512) + EPS)
    grad_mean = grad_sum * (1.0 / 512)
    product_mean = inv_std * product * (1.0 / 512)
    normed = (attended - mean) * inv_std
    scaled = normed * gain
    mixed = (scaled * gates).astype(BF16)
    grad_gate = (grads * scaled).astype(BF16)
    attended_grad = inv_std * (normed_grad - grad_mean - normed * product_mean)
    attended_grad = jnp.where(alive, attended_grad, 0.0).astype(BF16)
    dot_ref[0:64] = jnp.zeros_like(attended_grad)
    dot_ref[64:128] = attended_grad
    for s in range(HALF):
        mix_send[s, 0:64] = mixed[:, s * 128:(s + 1) * 128]
        mix_send[s, 64:128] = grad_gate[:, s * 128:(s + 1) * 128]
    mix_got[h] = mix_send[h]
    sent += to_half(mix_send, mix_got, mix_ss, mix_rs)

    for d in range(NX):
        relay_arrival(d).wait_recv()
    for n in range(2 * NYL):
        part = nn(mixed, cot_all[:, :, n * 128:(n + 1) * 128].reshape(HALF * ROWS, 128))
        y_own[n] = part
        y_send[n] = part.astype(BF16)
    to_y = []
    for d in range(1, 2 * NYL):
        to = (y + d) % (2 * NYL)
        copy = remote(
            y_send.at[to], y_got.at[d], y_ss.at[d], y_rs.at[d],
            device(to % NYL, z, to // NYL, x, core),
        )
        copy.start()
        to_y.append(copy)

    def columns_of(i):
        return pl.ds(pl.multiple_of(i * TILE, TILE), TILE)

    def backward_tile(i, kv, diagonal):
        qs, dots = (qf[rows_of(i)], dot_ref[:, columns_of(i)])
        half_score = nt(kv, qs)
        grad = nn(kv, dots)
        tanh = jnp.tanh(half_score)
        plus = 1.0 + tanh
        weight = half_score * plus
        slope = grad * (plus + weight * (1.0 - tanh))
        if diagonal:
            keep = tile_row <= tile_col
            weight = jnp.where(keep, weight, 0.0)
            slope = jnp.where(keep, slope, 0.0)
        slope = slope.astype(BF16)
        dqt_acc[i] += tn(kv[:, :64], slope)
        return nn(slope, qs) + nt(weight.astype(BF16), dots)

    def down_copy(s):
        return remote(down_send.at[s], down_got.at[h], down_ss.at[s], down_rs.at[h], (g, s))

    def down_arrival(t):
        return remote(
            down_send.at[t], down_got.at[t], down_ss.at[t], down_rs.at[t], (g, HALF + t)
        )

    @pl.when(upper)
    def _():
        for j in range(2):
            up_acc[...] = jnp.zeros_like(up_acc)

            @pl.loop(0, 2)
            def _(i):
                up_acc[...] += backward_tile(i, upper_kv(j), False)

            for s in range(4):
                down_send[4 * j + s] = up_acc[s * 128:(s + 1) * 128].astype(BF16)
                down_copy(4 * j + s).start()

    @pl.loop(0, 2)
    def _(i):
        dkv_acc[rows_of(i)] += backward_tile(i, local_kv(i), True)

    dkv_acc[0:TILE] += backward_tile(1, local_kv(0), False)

    for s in range(HALF):
        i, at = (s // 4, (s % 4) * 128)
        back_send[s, 0:64] = (dqt_acc[i, :, at:at + 128] * 0.0625).astype(BF16)
        back_send[s, 64:192] = dkv_acc[s * 128:(s + 1) * 128].astype(BF16)
    back_got[h] = back_send[h]
    sent += to_half(back_send, back_got, back_ss, back_rs)

    total = y_own[y]
    for d in range(1, 2 * NYL):
        to_y[d - 1].wait_recv()
        total = total + y_got[d].astype(F32)
    near_all[z % ZA] = total.astype(BF16)
    for d in range(1, ZA):
        copy = remote(
            near_all.at[z % ZA], near_all.at[z % ZA], near_ss.at[d], near_rs.at[d],
            device(y_lo, near_z(z, d), y_hi, x, core),
        )
        copy.start()
        sent.append(copy)

    from_half(mix_send, mix_got, mix_ss, mix_rs)
    whole = jnp.concatenate([mix_got[t, 0:64] for t in range(HALF)], axis=0)
    out_ref[...] = tn(whole, weight_ref[...]).astype(BF16)
    for p in range(HALF // 2):
        pair = jnp.concatenate(
            [mix_got[2 * p, 64:128].astype(F32), mix_got[2 * p + 1, 64:128].astype(F32)], axis=0
        )
        gg_ref[:, p * 128:(p + 1) * 128] = pair.T.astype(BF16)

    for d in range(1, ZA):
        remote(
            near_all.at[z % ZA], near_all.at[(z % ZA + ZA - d) % ZA], near_ss.at[d], near_rs.at[d],
            device(y_lo, near_z(z, d), y_hi, x, core),
        ).wait_recv()
    total = near_all[0].astype(F32)
    for n in range(1, ZA):
        total = total + near_all[n].astype(F32)
    far_all[z // ZA] = total.astype(BF16)
    for d in range(1, ZB):
        copy = remote(
            far_all.at[z // ZA], far_all.at[z // ZA], far_ss.at[d], far_rs.at[d],
            device(y_lo, far_z(z, d), y_hi, x, core),
        )
        copy.start()
        sent.append(copy)

    from_half(back_send, back_got, back_ss, back_rs)
    for p in range(HALF // 2):
        pair = jnp.concatenate(
            [back_got[2 * p, 0:64].astype(F32), back_got[2 * p + 1, 0:64].astype(F32)], axis=0
        )
        gq_ref[:, p * 128:(p + 1) * 128] = pair.T.astype(BF16)

    for d in range(1, ZB):
        remote(
            far_all.at[z // ZA], far_all.at[(z // ZA + ZB - d) % ZB], far_ss.at[d], far_rs.at[d],
            device(y_lo, far_z(z, d), y_hi, x, core),
        ).wait_recv()
    total = far_all[0].astype(F32)
    for n in range(1, ZB):
        total = total + far_all[n].astype(F32)
    fin_send[...] = total.astype(BF16)

    def fin_copy(lo, cc):
        return remote(
            fin_send, fin_got.at[h], fin_ss.at[lo * 2 + cc], fin_rs.at[h],
            device(lo, z, y_hi, y_lo, cc),
        )

    def not_me(lo, cc):
        return (x != y_lo) | (lo != y_lo) | (cc != core)

    for lo in range(NYL):
        for cc in range(2):

            @pl.when(not_me(lo, cc))
            def _():
                fin_copy(lo, cc).start()

    @pl.when(x == y_lo)
    def _():
        fin_got[h] = fin_send[...]

    @pl.when(lower)
    def _():
        for t in range(HALF):
            down_arrival(t).wait_recv()

    for p in range(HALF // 2):
        cols = slice(p * 128, (p + 1) * 128)
        heads = []
        for t in (2 * p, 2 * p + 1):
            mine = back_got[t, 64:192].astype(F32)
            far = jnp.where(lower, down_got[t].astype(F32), 0.0)
            heads.append(mine + far)
        kk, vv = join_heads(*heads)
        gk_ref[:, cols] = kk.astype(BF16)
        gv_ref[:, cols] = vv.astype(BF16)

    for xx in range(NX):
        for cc in range(2):
            t = xx * 2 + cc

            @pl.when((x != y_lo) | (h != t))
            def _():
                remote(
                    fin_send, fin_got.at[t], fin_ss.at[t], fin_rs.at[t],
                    device(x, z, y_hi, xx, cc),
                ).wait_recv()

    for p in range(HALF // 2):
        pair = jnp.concatenate(
            [fin_got[2 * p].astype(F32), fin_got[2 * p + 1].astype(F32)], axis=0
        )
        fin_turned[:, p * 128:(p + 1) * 128] = pair.T
    gw_ref[...] = fin_turned[pl.ds(pl.multiple_of(core * 64, 64), 64)]

    for copy in sent + to_y:
        copy.wait_send()
    for lo in range(NYL):
        for cc in range(2):

            @pl.when(not_me(lo, cc))
            def _():
                fin_copy(lo, cc).wait_send()

    @pl.when(lower)
    def _():
        for t in range(HALF):
            up_copy(t).wait_send()

    @pl.when(upper)
    def _():
        for s in range(HALF):
            down_copy(s).wait_send()


def shards(query, key, value, gate_u, out_grad, lengths, norm_gain, out_weight):
    dma = pltpu.SemaphoreType.DMA
    vmem = pltpu.VMEM
    rows = query.shape[0]
    outs = [((rows, 1024), BF16)] + [((rows, 512), BF16)] * 4 + [((64, 512), F32)]
    results = pl.pallas_call(
        layer_kernel,
        out_shape=tuple(vmem(*out) for out in outs),
        in_specs=[pl.BlockSpec(memory_space=pl.ANY)] * 8,
        out_specs=(pl.BlockSpec(memory_space=vmem),) * 6,
        scratch_shapes=[
            vmem((ROWS, 512), BF16),
            vmem((ROWS, 512), BF16),
            vmem((ROWS, 512), BF16),
            vmem((ROWS, 512), BF16),
            pltpu.SMEM((1,), jnp.int32),
            vmem((1, 512), F32),
            vmem((512, 1024), BF16),
            vmem((HALF, 192, 128), BF16),
            vmem((HALF, 192, 128), BF16),
            vmem((HALF, 128, 128), BF16),
            vmem((HALF, 128, 128), BF16),
            vmem((HALF, 128, 128), BF16),
            vmem((HALF, ROWS, 1024), BF16),
            vmem((HALF, 64, 128), F32),
            vmem((1024, 128), BF16),
            vmem((128, 1024), BF16),
            vmem((2, 64, TILE), F32),
            vmem((8, TILE), F32),
            vmem((HALF, 8, TILE), F32),
            vmem((HALF, 128, 128), BF16),
            vmem((HALF, 128, 128), BF16),
            vmem((1024, 128), F32),
            vmem((2, 64, TILE), F32),
            vmem((TILE, 128), F32),
            vmem((HALF, 192, 128), BF16),
            vmem((HALF, 192, 128), BF16),
            vmem((HALF, 128, 128), BF16),
            vmem((HALF, 128, 128), BF16),
            vmem((2 * NYL, 64, 128), F32),
            vmem((2 * NYL, 64, 128), BF16),
            vmem((2 * NYL, 64, 128), BF16),
            vmem((ZA, 64, 128), BF16),
            vmem((ZB, 64, 128), BF16),
            vmem((64, 128), BF16),
            vmem((HALF, 64, 128), BF16),
            vmem((128, 512), F32),
        ]
        + [dma((HALF,))] * 27,
        compiler_params=pltpu.CompilerParams(collective_id=0, has_side_effects=True),
    )(query, key, value, gate_u, out_grad, lengths, norm_gain.reshape(1, 512), out_weight)
    anywhere = pl.BlockSpec(memory_space=pl.ANY)
    results = pl.pallas_call(
        store_kernel,
        out_shape=tuple(jax.ShapeDtypeStruct(*out) for out in outs),
        in_specs=[pl.BlockSpec(memory_space=vmem)] * 6,
        out_specs=(anywhere,) * 6,
        scratch_shapes=[dma((6,))],
    )(*[pltpu.with_memory_space_constraint(one, vmem) for one in results])
    return (*results[:5], results[5].T)


def store_kernel(*refs):
    sources, targets, sems = (refs[:6], refs[6:12], refs[12])
    copies = [
        pltpu.make_async_copy(source, target, sems.at[n])
        for n, (source, target) in enumerate(zip(sources, targets))
    ]
    for copy in copies:
        copy.start()
    for copy in copies:
        copy.wait()


def solution(mesh):
    split = P(("grp", "blk"), None)
    return jax.shard_map(
        shards,
        mesh=mesh,
        in_specs=(split,) * 5 + (P("grp"), P(), P()),
        out_specs=(split,) * 5 + (P(None, "blk"),),
        check_vma=False,
    )
```

```python
import jax
import jax.numpy as jnp
from jax import lax
from jax.experimental import pallas as pl
from jax.experimental.pallas import tpu as pltpu
from jax.sharding import PartitionSpec as P

MESH = pl.DeviceIdType.MESH
EPS = 1e-05
ZA = 4
ZB = 3
NZ = ZA * ZB
NYL = 4
NX = 4
HALF = 8
ROWS = 128
TILE = 512
F32 = jnp.float32
BF16 = jnp.bfloat16


def where_am_i():
    g, b = (lax.axis_index("grp"), lax.axis_index("blk"))
    return (g // NZ, g % NZ, b // 8, (b // 2) % NX, b % 2)


def device(y_lo, z, y_hi, x, core):
    return (y_lo * NZ + z, (y_hi * NX + x) * 2 + core)


def remote(src, dst, send_sem, recv_sem, target):
    return pltpu.make_async_remote_copy(
        src_ref=src, dst_ref=dst, send_sem=send_sem, recv_sem=recv_sem,
        device_id=target, device_id_type=MESH,
    )


def swap(part):
    return pltpu.roll(part.astype(F32), 64, 1)


def low_lanes(rows):
    return lax.broadcasted_iota(jnp.int32, (rows, 128), 1) < 64


def fold_rows(block, odd):
    low = low_lanes(64)
    top, bottom = (block[:64], block[64:])
    if odd:
        return jnp.where(low, swap(top), bottom.astype(F32))
    return jnp.where(low, top.astype(F32), swap(bottom))


def join_heads(even, odd):
    low = low_lanes(even.shape[0])
    return (jnp.where(low, even, swap(odd)), jnp.where(low, swap(even), odd))


def nt(left, right):
    return lax.dot_general(left, right, (((1,), (1,)), ((), ())), preferred_element_type=F32)


def tn(left, right):
    return lax.dot_general(left, right, (((0,), (0,)), ((), ())), preferred_element_type=F32)


def nn(left, right):
    return jnp.dot(left, right, preferred_element_type=F32)


def symmetric_partners(me):
    y_lo, z, y_hi, x, core = me
    mine = (y_hi * NX + x) * 2 + core
    y = y_hi * NYL + y_lo
    found = [(y_lo * NZ + z, (mine + d) % 16) for d in range(1, 16)]
    for d in range(1, 2 * NYL):
        if d != NYL:
            to = (y + d) % (2 * NYL)
            found.append(device(to % NYL, z, to // NYL, x, core))
    for d in range(1, ZA):
        found.append(device(y_lo, near_z(z, d), y_hi, x, core))
    for d in range(1, ZB):
        found.append(device(y_lo, far_z(z, d), y_hi, x, core))
    for d in range(1, NYL):
        for cc in range(2):
            found.append(device((y_lo + d) % NYL, z, y_hi, y_lo, cc))
    return found


def near_z(z, d):
    return z // ZA * ZA + (z % ZA + d) % ZA


def far_z(z, d):
    return (z // ZA + d) % ZB * ZA + z % ZA


def layer_kernel(
    q_hbm, k_hbm, v_hbm, gate_hbm, cot_hbm, length_hbm, gain_hbm, weight_hbm,
    out_ref, gq_ref, gk_ref, gv_ref, gg_ref, gw_ref,
    q_ref, k_ref, v_ref, gate_ref, length_ref, gain_ref, weight_ref,
    in_send, in_got, side_send, side_got, up_got, cot_all, gain_cols,
    qf, dot_ref, att_acc, stat_send, stat_got, mix_send, mix_got,
    dkv_acc, dqt_acc, up_acc, back_send, back_got, down_send, down_got,
    y_own, y_send, y_got, near_all, far_all, fin_send, fin_got, fin_turned,
    load, in_ss, in_rs, side_ss, side_rs, up_ss, up_rs, cot_ss, cot_rs, rel_ss, rel_rs,
    stat_ss, stat_rs, mix_ss, mix_rs, back_ss, back_rs, down_ss, down_rs,
    y_ss, y_rs, near_ss, near_rs, far_ss, far_rs, fin_ss, fin_rs,
):
    me = where_am_i()
    y_lo, z, y_hi, x, core = me
    g = y_lo * NZ + z
    y = y_hi * NYL + y_lo
    h = x * 2 + core
    base = y_hi * HALF
    upper = y_hi == 1
    lower = y_hi == 0

    loads = [
        pltpu.make_async_copy(k_hbm, k_ref, load.at[0]),
        pltpu.make_async_copy(v_hbm, v_ref, load.at[1]),
        pltpu.make_async_copy(q_hbm, q_ref, load.at[2]),
        pltpu.make_async_copy(gate_hbm, gate_ref, load.at[3]),
        pltpu.make_async_copy(cot_hbm, cot_all.at[h], load.at[4]),
        pltpu.make_async_copy(weight_hbm, weight_ref, load.at[5]),
        pltpu.make_async_copy(gain_hbm, gain_ref, load.at[6]),
        pltpu.make_async_copy(length_hbm, length_ref, load.at[7]),
    ]
    for copy in loads:
        copy.start()

    def far_sources():
        return [device(x, z, y_hi, xx, cc) for xx in range(NX) for cc in range(2)]

    barrier = pltpu.get_barrier_semaphore()
    partners = symmetric_partners(me)
    for target in partners:
        pl.semaphore_signal(barrier, inc=1, device_id=target, device_id_type=MESH)

    @pl.when(x != y_lo)
    def _():
        for target in far_sources():
            pl.semaphore_signal(barrier, inc=1, device_id=target, device_id_type=MESH)

    for copy in loads[:3]:
        copy.wait()
    low128 = low_lanes(128)
    for t in range(HALF):
        cols = slice((t // 2) * 128, (t // 2 + 1) * 128)
        kk, vv = (k_ref[:, cols], v_ref[:, cols])
        if t % 2:
            pair = jnp.where(low128, swap(kk), vv.astype(F32))
        else:
            pair = jnp.where(low128, kk.astype(F32), swap(vv))
        in_send[t, 64:192] = pair.astype(BF16)
        in_send[t, 0:64] = (fold_rows(q_ref[:, cols], t % 2) * 0.0625).astype(BF16)
    in_got[h] = in_send[h]

    @pl.when(x != y_lo)
    def _():
        pl.semaphore_wait(barrier, len(partners) + HALF)

    @pl.when(x == y_lo)
    def _():
        pl.semaphore_wait(barrier, len(partners))

    def up_copy(t):
        return remote(
            in_send.at[t, pl.ds(64, 128)], up_got.at[h], up_ss.at[t], up_rs.at[h], (g, HALF + t)
        )

    def up_arrival(s):
        return remote(
            in_send.at[s, pl.ds(64, 128)], up_got.at[s], up_ss.at[s], up_rs.at[s], (g, s)
        )

    def heads_at(d):
        return [(x + d) % NX * 2 + cc for cc in range(2)]

    @pl.when(lower)
    def _():
        for t in heads_at(0):
            up_copy(t).start()

    def to_half(send, got, ssem, rsem):
        copies = []
        for d in range(1, HALF):
            t = (h + d) % HALF
            copies.append(remote(send.at[t], got.at[h], ssem.at[d], rsem.at[d], (g, base + t)))
        for copy in copies:
            copy.start()
        return copies

    def from_half(send, got, ssem, rsem):
        for d in range(1, HALF):
            t = (h + d) % HALF
            s = (h + HALF - d) % HALF
            remote(send.at[t], got.at[s], ssem.at[d], rsem.at[d], (g, base + t)).wait_recv()

    sent = to_half(in_send, in_got, in_ss, in_rs)

    @pl.when(lower)
    def _():
        for d in (1, 3, 2):
            for t in heads_at(d):
                up_copy(t).start()

    for copy in loads[3:7]:
        copy.wait()
    for p in range(HALF // 2):
        cols = slice(p * 128, (p + 1) * 128)
        turned = gate_ref[:, cols].astype(F32).T.astype(BF16)
        side_send[2 * p, 0:64] = turned[:64]
        side_send[2 * p + 1, 0:64] = turned[64:]
        spread = jnp.broadcast_to(gain_ref[:, cols], (128, 128)).T
        gain_cols[2 * p] = spread[:64]
        gain_cols[2 * p + 1] = spread[64:]
        grads = nt(weight_ref[cols], cot_all[h]).astype(BF16)
        side_send[2 * p, 64:128] = grads[:64]
        side_send[2 * p + 1, 64:128] = grads[64:]
    side_got[h] = side_send[h]
    sent += to_half(side_send, side_got, side_ss, side_rs)

    sister = (g, base + h + 1 - 2 * core)

    def slot_of(d):
        return (x + NX - d) % NX * 2 + core

    def to_chip(part, d, n):
        return remote(
            part, part, cot_ss.at[n], cot_rs.at[n], device(y_lo, z, y_hi, (x + d) % NX, core)
        )

    for d in (1, 3):
        copy = to_chip(cot_all.at[h], d, d)
        copy.start()
        sent.append(copy)

    def relay(d):
        slot = (x + NX - d) % NX * 2 + core
        return remote(cot_all.at[slot], cot_all.at[slot], rel_ss.at[d], rel_rs.at[d], sister)

    def relay_arrival(d):
        slot = (x + NX - d) % NX * 2 + 1 - core
        return remote(cot_all.at[slot], cot_all.at[slot], rel_ss.at[d], rel_rs.at[d], sister)

    first = relay(0)
    first.start()
    sent.append(first)

    from_half(in_send, in_got, in_ss, in_rs)
    low64 = low_lanes(64)
    for s in range(HALF):
        folded = in_got[s, 0:64].astype(F32)
        qf[s * 128:s * 128 + 64] = jnp.where(low64, folded, 0.0).astype(BF16)
        qf[s * 128 + 64:s * 128 + 128] = jnp.where(low64, swap(folded), 0.0).astype(BF16)
    att_acc[...] = jnp.zeros_like(att_acc)
    dkv_acc[...] = jnp.zeros_like(dkv_acc)
    dqt_acc[...] = jnp.zeros_like(dqt_acc)

    def local_kv(j):
        return in_got[pl.ds(j * 4, 4), 64:192].reshape(TILE, 128)

    def upper_kv(j):
        return up_got[pl.ds(j * 4, 4)].reshape(TILE, 128)

    def rows_of(i):
        return pl.ds(pl.multiple_of(i * TILE, TILE), TILE)

    tile_row = lax.broadcasted_iota(jnp.int32, (TILE, TILE), 0)
    tile_col = lax.broadcasted_iota(jnp.int32, (TILE, TILE), 1)

    def forward_tile(i, kv, diagonal):
        half_score = nt(kv, qf[rows_of(i)])
        weight = half_score + half_score * jnp.tanh(half_score)
        if diagonal:
            weight = jnp.where(tile_row <= tile_col, weight, 0.0)
        att_acc[i] += tn(kv[:, 64:], weight.astype(BF16))

    @pl.loop(0, 2)
    def _(i):
        forward_tile(i, local_kv(i), True)

    forward_tile(1, local_kv(0), False)
    to_chip(cot_all.at[slot_of(1)], 1, 1).wait_recv()
    to_chip(cot_all.at[slot_of(3)], 3, 3).wait_recv()
    for copy in (
        to_chip(cot_all.at[slot_of(1), pl.ds(0, 64)], 1, 4),
        to_chip(cot_all.at[slot_of(3), pl.ds(64, 64)], 3, 5),
        relay(1),
        relay(3),
    ):
        copy.start()
        sent.append(copy)
    from_half(side_send, side_got, side_ss, side_rs)
    loads[7].wait()
    gates = jnp.concatenate([side_got[s, 0:64] for s in range(HALF)], axis=1).astype(F32)
    grads = jnp.concatenate([side_got[s, 64:128] for s in range(HALF)], axis=1).astype(F32)
    gain = gain_cols[h][:, 0:1]
    normed_grad = grads * gates * gain
    position = base * ROWS + lax.broadcasted_iota(jnp.int32, (1, HALF * ROWS), 1)
    alive = position < length_ref[0]

    @pl.when(upper)
    def _():
        for j in range(2):
            for s in range(4):
                up_arrival(4 * j + s).wait_recv()

            @pl.loop(0, 2)
            def _(i):
                forward_tile(i, upper_kv(j), False)

    attended = jnp.where(alive, jnp.concatenate([att_acc[0], att_acc[1]], axis=1), 0.0)
    mean_mine = jnp.sum(attended, axis=0, keepdims=True) * (1.0 / 64)
    centre = attended - mean_mine
    stats = (
        mean_mine,
        jnp.sum(centre * centre, axis=0, keepdims=True),
        jnp.sum(normed_grad, axis=0, keepdims=True),
        jnp.sum(normed_grad * centre, axis=0, keepdims=True),
    )
    for n, stat in enumerate(stats):
        stat_send[n:n + 1] = stat[:, :TILE]
        stat_send[n + 4:n + 5] = stat[:, TILE:]
    stat_got[h] = stat_send[...]
    for d in range(1, HALF):
        t = (h + d) % HALF
        copy = remote(stat_send, stat_got.at[h], stat_ss.at[d], stat_rs.at[d], (g, base + t))
        copy.start()
        sent.append(copy)
    to_chip(cot_all.at[slot_of(2), pl.ds(0, 64)], 1, 4).wait_recv()
    to_chip(cot_all.at[slot_of(2), pl.ds(64, 64)], 3, 5).wait_recv()
    copy = relay(2)
    copy.start()
    sent.append(copy)
    for d in range(1, HALF):
        t = (h + d) % HALF
        s = (h + HALF - d) % HALF
        remote(
            stat_send, stat_got.at[s], stat_ss.at[d], stat_rs.at[d], (g, base + t)
        ).wait_recv()

    def stat_rows(n):
        return [
            jnp.concatenate([stat_got[s, n:n + 1], stat_got[s, n + 4:n + 5]], axis=1)
            for s in range(HALF)
        ]

    means, squares, sums, products = (stat_rows(n) for n in range(4))
    mean = sum(means) * (1.0 / HALF)
    square = sum(squares)
    grad_sum = sum(sums)
    product = sum(products)
    for s in range(HALF):
        off = means[s] - mean
        square = square + 64.0 * (off * off)
        product = product + off * sums[s]
    inv_std = lax.rsqrt(square * (1.0 / 512) + EPS)
    grad_mean = grad_sum * (1.0 / 512)
    product_mean = inv_std * product * (1.0 / 512)
    normed = (attended - mean) * inv_std
    scaled = normed * gain
    mixed = (scaled * gates).astype(BF16)
    grad_gate = (grads * scaled).astype(BF16)
    attended_grad = inv_std * (normed_grad - grad_mean - normed * product_mean)
    attended_grad = jnp.where(alive, attended_grad, 0.0).astype(BF16)
    dot_ref[0:64] = jnp.zeros_like(attended_grad)
    dot_ref[64:128] = attended_grad
    for s in range(HALF):
        mix_send[s, 0:64] = mixed[:, s * 128:(s + 1) * 128]
        mix_send[s, 64:128] = grad_gate[:, s * 128:(s + 1) * 128]
    mix_got[h] = mix_send[h]
    sent += to_half(mix_send, mix_got, mix_ss, mix_rs)

    for d in range(NX):
        relay_arrival(d).wait_recv()
    for n in range(2 * NYL):
        part = nn(mixed, cot_all[:, :, n * 128:(n + 1) * 128].reshape(HALF * ROWS, 128))
        y_own[n] = part
        y_send[n] = part.astype(BF16)
    to_y = []
    for d in range(1, 2 * NYL):
        to = (y + d) % (2 * NYL)
        copy = remote(
            y_send.at[to], y_got.at[d], y_ss.at[d], y_rs.at[d],
            device(to % NYL, z, to // NYL, x, core),
        )
        copy.start()
        to_y.append(copy)

    def columns_of(i):
        return pl.ds(pl.multiple_of(i * TILE, TILE), TILE)

    def backward_tile(i, kv, diagonal):
        qs, dots = (qf[rows_of(i)], dot_ref[:, columns_of(i)])
        half_score = nt(kv, qs)
        grad = nn(kv, dots)
        tanh = jnp.tanh(half_score)
        plus = 1.0 + tanh
        weight = half_score * plus
        slope = grad * (plus + weight * (1.0 - tanh))
        if diagonal:
            keep = tile_row <= tile_col
            weight = jnp.where(keep, weight, 0.0)
            slope = jnp.where(keep, slope, 0.0)
        slope = slope.astype(BF16)
        dqt_acc[i] += tn(kv[:, :64], slope)
        return nn(slope, qs) + nt(weight.astype(BF16), dots)

    def down_copy(s):
        return remote(down_send.at[s], down_got.at[h], down_ss.at[s], down_rs.at[h], (g, s))

    def down_arrival(t):
        return remote(
            down_send.at[t], down_got.at[t], down_ss.at[t], down_rs.at[t], (g, HALF + t)
        )

    @pl.when(upper)
    def _():
        for j in range(2):
            up_acc[...] = jnp.zeros_like(up_acc)

            @pl.loop(0, 2)
            def _(i):
                up_acc[...] += backward_tile(i, upper_kv(j), False)

            for s in range(4):
                down_send[4 * j + s] = up_acc[s * 128:(s + 1) * 128].astype(BF16)

    @pl.loop(0, 2)
    def _(i):
        dkv_acc[rows_of(i)] += backward_tile(i, local_kv(i), True)

    dkv_acc[0:TILE] += backward_tile(1, local_kv(0), False)

    for s in range(HALF):
        i, at = (s // 4, (s % 4) * 128)
        back_send[s, 0:64] = (dqt_acc[i, :, at:at + 128] * 0.0625).astype(BF16)
        back_send[s, 64:192] = dkv_acc[s * 128:(s + 1) * 128].astype(BF16)
    back_got[h] = back_send[h]
    sent += to_half(back_send, back_got, back_ss, back_rs)

    @pl.when(upper)
    def _():
        for d in (0, 1, 3, 2):
            for s in heads_at(d):
                down_copy(s).start()

    total = y_own[y]
    for d in range(1, 2 * NYL):
        to_y[d - 1].wait_recv()
        total = total + y_got[d].astype(F32)
    near_all[z % ZA] = total.astype(BF16)
    for d in range(1, ZA):
        copy = remote(
            near_all.at[z % ZA], near_all.at[z % ZA], near_ss.at[d], near_rs.at[d],
            device(y_lo, near_z(z, d), y_hi, x, core),
        )
        copy.start()
        sent.append(copy)

    from_half(mix_send, mix_got, mix_ss, mix_rs)
    whole = jnp.concatenate([mix_got[t, 0:64] for t in range(HALF)], axis=0)
    out_ref[...] = tn(whole, weight_ref[...]).astype(BF16)
    for p in range(HALF // 2):
        pair = jnp.concatenate(
            [mix_got[2 * p, 64:128].astype(F32), mix_got[2 * p + 1, 64:128].astype(F32)], axis=0
        )
        gg_ref[:, p * 128:(p + 1) * 128] = pair.T.astype(BF16)

    for d in range(1, ZA):
        remote(
            near_all.at[z % ZA], near_all.at[(z % ZA + ZA - d) % ZA], near_ss.at[d], near_rs.at[d],
            device(y_lo, near_z(z, d), y_hi, x, core),
        ).wait_recv()
    total = near_all[0].astype(F32)
    for n in range(1, ZA):
        total = total + near_all[n].astype(F32)
    far_all[z // ZA] = total.astype(BF16)
    for d in range(1, ZB):
        copy = remote(
            far_all.at[z // ZA], far_all.at[z // ZA], far_ss.at[d], far_rs.at[d],
            device(y_lo, far_z(z, d), y_hi, x, core),
        )
        copy.start()
        sent.append(copy)

    for d in range(1, ZB):
        remote(
            far_all.at[z // ZA], far_all.at[(z // ZA + ZB - d) % ZB], far_ss.at[d], far_rs.at[d],
            device(y_lo, far_z(z, d), y_hi, x, core),
        ).wait_recv()
    total = far_all[0].astype(F32)
    for n in range(1, ZB):
        total = total + far_all[n].astype(F32)
    fin_send[...] = total.astype(BF16)

    def fin_copy(lo, cc):
        return remote(
            fin_send, fin_got.at[h], fin_ss.at[lo * 2 + cc], fin_rs.at[h],
            device(lo, z, y_hi, y_lo, cc),
        )

    def not_me(lo, cc):
        return (x != y_lo) | (lo != y_lo) | (cc != core)

    for lo in range(NYL):
        for cc in range(2):

            @pl.when(not_me(lo, cc))
            def _():
                fin_copy(lo, cc).start()

    @pl.when(x == y_lo)
    def _():
        fin_got[h] = fin_send[...]

    from_half(back_send, back_got, back_ss, back_rs)
    for p in range(HALF // 2):
        pair = jnp.concatenate(
            [back_got[2 * p, 0:64].astype(F32), back_got[2 * p + 1, 0:64].astype(F32)], axis=0
        )
        gq_ref[:, p * 128:(p + 1) * 128] = pair.T.astype(BF16)

    @pl.when(lower)
    def _():
        for t in range(HALF):
            down_arrival(t).wait_recv()

    for p in range(HALF // 2):
        cols = slice(p * 128, (p + 1) * 128)
        heads = []
        for t in (2 * p, 2 * p + 1):
            mine = back_got[t, 64:192].astype(F32)
            far = jnp.where(lower, down_got[t].astype(F32), 0.0)
            heads.append(mine + far)
        kk, vv = join_heads(*heads)
        gk_ref[:, cols] = kk.astype(BF16)
        gv_ref[:, cols] = vv.astype(BF16)

    for xx in range(NX):
        for cc in range(2):
            t = xx * 2 + cc

            @pl.when((x != y_lo) | (h != t))
            def _():
                remote(
                    fin_send, fin_got.at[t], fin_ss.at[t], fin_rs.at[t],
                    device(x, z, y_hi, xx, cc),
                ).wait_recv()

    for p in range(HALF // 2):
        pair = jnp.concatenate(
            [fin_got[2 * p].astype(F32), fin_got[2 * p + 1].astype(F32)], axis=0
        )
        fin_turned[:, p * 128:(p + 1) * 128] = pair.T
    gw_ref[...] = fin_turned[pl.ds(pl.multiple_of(core * 64, 64), 64)]

    for copy in sent + to_y:
        copy.wait_send()
    for lo in range(NYL):
        for cc in range(2):

            @pl.when(not_me(lo, cc))
            def _():
                fin_copy(lo, cc).wait_send()

    @pl.when(lower)
    def _():
        for t in range(HALF):
            up_copy(t).wait_send()

    @pl.when(upper)
    def _():
        for s in range(HALF):
            down_copy(s).wait_send()


def shards(query, key, value, gate_u, out_grad, lengths, norm_gain, out_weight):
    dma = pltpu.SemaphoreType.DMA
    vmem = pltpu.VMEM
    rows = query.shape[0]
    outs = [((rows, 1024), BF16)] + [((rows, 512), BF16)] * 4 + [((64, 512), F32)]
    results = pl.pallas_call(
        layer_kernel,
        out_shape=tuple(vmem(*out) for out in outs),
        in_specs=[pl.BlockSpec(memory_space=pl.ANY)] * 8,
        out_specs=(pl.BlockSpec(memory_space=vmem),) * 6,
        scratch_shapes=[
            vmem((ROWS, 512), BF16),
            vmem((ROWS, 512), BF16),
            vmem((ROWS, 512), BF16),
            vmem((ROWS, 512), BF16),
            pltpu.SMEM((1,), jnp.int32),
            vmem((1, 512), F32),
            vmem((512, 1024), BF16),
            vmem((HALF, 192, 128), BF16),
            vmem((HALF, 192, 128), BF16),
            vmem((HALF, 128, 128), BF16),
            vmem((HALF, 128, 128), BF16),
            vmem((HALF, 128, 128), BF16),
            vmem((HALF, ROWS, 1024), BF16),
            vmem((HALF, 64, 128), F32),
            vmem((1024, 128), BF16),
            vmem((128, 1024), BF16),
            vmem((2, 64, TILE), F32),
            vmem((8, TILE), F32),
            vmem((HALF, 8, TILE), F32),
            vmem((HALF, 128, 128), BF16),
            vmem((HALF, 128, 128), BF16),
            vmem((1024, 128), F32),
            vmem((2, 64, TILE), F32),
            vmem((TILE, 128), F32),
            vmem((HALF, 192, 128), BF16),
            vmem((HALF, 192, 128), BF16),
            vmem((HALF, 128, 128), BF16),
            vmem((HALF, 128, 128), BF16),
            vmem((2 * NYL, 64, 128), F32),
            vmem((2 * NYL, 64, 128), BF16),
            vmem((2 * NYL, 64, 128), BF16),
            vmem((ZA, 64, 128), BF16),
            vmem((ZB, 64, 128), BF16),
            vmem((64, 128), BF16),
            vmem((HALF, 64, 128), BF16),
            vmem((128, 512), F32),
        ]
        + [dma((HALF,))] * 27,
        compiler_params=pltpu.CompilerParams(collective_id=0, has_side_effects=True),
    )(query, key, value, gate_u, out_grad, lengths, norm_gain.reshape(1, 512), out_weight)
    anywhere = pl.BlockSpec(memory_space=pl.ANY)
    results = pl.pallas_call(
        store_kernel,
        out_shape=tuple(jax.ShapeDtypeStruct(*out) for out in outs),
        in_specs=[pl.BlockSpec(memory_space=vmem)] * 6,
        out_specs=(anywhere,) * 6,
        scratch_shapes=[dma((6,))],
    )(*[pltpu.with_memory_space_constraint(one, vmem) for one in results])
    return (*results[:5], results[5].T)


def store_kernel(*refs):
    sources, targets, sems = (refs[:6], refs[6:12], refs[12])
    copies = [
        pltpu.make_async_copy(source, target, sems.at[n])
        for n, (source, target) in enumerate(zip(sources, targets))
    ]
    for copy in copies:
        copy.start()
    for copy in copies:
        copy.wait()


def solution(mesh):
    split = P(("grp", "blk"), None)
    return jax.shard_map(
        shards,
        mesh=mesh,
        in_specs=(split,) * 5 + (P("grp"), P(), P()),
        out_specs=(split,) * 5 + (P(None, "blk"),),
        check_vma=False,
    )
```
